32 devices in a mesh: groups: 2 (over x), steps: 16 (over z, y, core).
Axes of the slice: x: 2, y: 2, z: 4, core: 2. Of those that a mesh axis runs over, the one named last changes fastest.
Arguments:
- states: float32 [32, 4, 4096], P(('groups', 'steps')), parts along dimension 0, may hold values from -6 to 6
- t_sched: int32 [66], P('groups'), parts along dimension 0, may hold values from 0 to 999, as said below
- advances: int32 [4], P('groups'), parts along dimension 0, may hold values from 1 to 16, as said below
- in_weight: bfloat16 [320, 4], replicated, may hold values from -3 to 3
- time_weight: float32 [320, 320], replicated, may hold values from -0.3125 to 0.3125
- mid_weight: bfloat16 [320, 320], replicated, may hold values from -0.3125 to 0.3125
- out_weight: bfloat16 [4, 320], replicated, may hold values from -0.3125 to 0.3125
Outputs:
- final_states: float32 [32, 4, 4096], P(('groups', 'steps')), parts along dimension 0
- errors: float32 [4, 4, 16], P('groups', None, 'steps'), parts along dimension 0
The draws below stay inside these ranges and needn't reach their ends.
There are 2 independent parts, one for each index of `groups`. The reference program is written for one: setup_inputs(seed, part) draws one part's arguments, and reference() takes and returns one part's arrays. A program takes and returns all parts, laid end to end along the dimension named above; an argument that names none is the same for every part. Nothing has to cross between parts.
Inputs may be any that keep to these rules, and one draw needn't show every extreme that they name: `t_sched`: strictly decreasing. Some round advances by exactly 16.
All inputs are finite; a program needn't handle non-finite values.
Results may differ from the reference program's by a relative error of at most 0.0024.
Values sent between devices are 32-bit elements; how exact they have to be, the bound alone decides.
A program may use at most 64 MiB of HBM per device.

```python
import math
import jax
import jax.numpy as jnp
from jax import lax

CH = 320
LAT = 4
TSTEPS = 1000
ROWS = 4096
ITERS = 4
ROUNDS = 2
WINDOW = 16
SCHED = 33
ADV_MOST = 16


def draw_t_sched(key, part):
    picked = jax.random.permutation(key, TSTEPS)[:SCHED].astype(jnp.int32)
    return -jnp.sort(-picked)


def draw_advances(key, part):
    first_key = jax.random.fold_in(key, 11)
    second_key = jax.random.fold_in(key, 12)
    values = jax.random.randint(first_key, (ROUNDS,), 1, ADV_MOST + 1).astype(jnp.int32)
    chosen = jax.random.randint(second_key, (), 0, ROUNDS)
    return jnp.where(jnp.arange(ROUNDS) == chosen, ADV_MOST, values).astype(jnp.int32)


def block_levels(key, dims, shards, low, high):
    loudness = 1.0
    for position, blocks in shards:
        draws = jax.random.uniform(jax.random.fold_in(jax.random.fold_in(key, 6), position), (blocks,), jnp.float32, low / len(shards), high / len(shards))
        loudness = loudness * jnp.repeat(jnp.exp(draws), dims[position] // blocks).reshape((-1,) + (1,) * (len(dims) - 1 - position))
    return loudness


def gaussian(stream_key, shape, width, limit, cuts=(), kind=jnp.bfloat16):
    entries = jax.random.normal(stream_key, shape, jnp.float32) * width
    if len(cuts) > 0:
        entries = block_levels(stream_key, shape, cuts, -0.22, 0.18) * entries
    return jnp.clip(entries, min=-limit, max=limit).astype(kind)


def setup_inputs(seed: int = 0, part: int = 0) -> dict:
    streams_of = jax.random.split(jax.random.key(seed), 8)
    own_keys = jax.random.split(jax.random.fold_in(streams_of[7], part), 8)
    states = gaussian(own_keys[0], (WINDOW, LAT, ROWS), 1.0, 6.0, ((0, 16),), jnp.float32)
    t_sched = draw_t_sched(jax.random.fold_in(jax.random.fold_in(streams_of[7], part), 71), part)
    advances = draw_advances(jax.random.fold_in(jax.random.fold_in(streams_of[7], part), 71), part)
    in_weight = gaussian(streams_of[3], (CH, LAT), LAT ** -0.5, 3.0)
    time_weight = gaussian(streams_of[4], (CH, CH), CH ** -0.5, 0.3125, (), jnp.float32)
    mid_weight = gaussian(streams_of[5], (CH, CH), CH ** -0.5, 0.3125)
    out_weight = gaussian(streams_of[6], (LAT, CH), CH ** -0.5, 0.3125)
    return dict(states=states, t_sched=t_sched, advances=advances, in_weight=in_weight, time_weight=time_weight, mid_weight=mid_weight, out_weight=out_weight)


def alpha_table():
    levels = jnp.arange(TSTEPS, dtype=jnp.float32)
    low = math.sqrt(0.00085)
    high = math.sqrt(0.012)
    betas = (low + (high - low) * levels / (TSTEPS - 1)) ** 2
    return jnp.exp(jnp.cumsum(jnp.log1p(-betas)))

def time_features(stamp):
    halfwidth = CH // 2
    freqs = jnp.exp(-math.log(10000.0) * jnp.arange(halfwidth, dtype=jnp.float32) / halfwidth)
    angles = stamp.astype(jnp.float32) * freqs
    return jnp.concatenate([jnp.cos(angles), jnp.sin(angles)])

def denoise(state, embed, in_weight, mid_weight, out_weight):
    pre = jnp.dot(in_weight, state.astype(jnp.bfloat16), preferred_element_type=jnp.float32) + embed[:, None]
    hidden_one = jax.nn.silu(pre).astype(jnp.bfloat16)
    mixed = jnp.dot(mid_weight, hidden_one, preferred_element_type=jnp.float32)
    hidden_two = (jax.nn.silu(mixed) + pre).astype(jnp.bfloat16)
    return jnp.dot(out_weight, hidden_two, preferred_element_type=jnp.float32)

def reference(states, t_sched, advances, in_weight, time_weight, mid_weight, out_weight):
    alphas = alpha_table()
    window = states.shape[0]
    places = jnp.arange(window, dtype=jnp.int32)
    current = states
    window_start = jnp.int32(0)
    error_rows = []
    for round_no in range(ROUNDS):
        stamp_now = t_sched[window_start + places]
        stamp_next = t_sched[window_start + places + 1]
        alpha_now = alphas[stamp_now]
        alpha_next = alphas[stamp_next]
        coef_one = jnp.sqrt(alpha_next / alpha_now)
        coef_two = jnp.sqrt(1.0 - alpha_next) - coef_one * jnp.sqrt(1.0 - alpha_now)
        feats = jax.vmap(time_features)(stamp_now)
        embeds = jnp.dot(feats, time_weight.T, precision=lax.Precision.HIGHEST)
        sweep_rows = []
        for sweep in range(ITERS):
            noise = lax.map(lambda pair: denoise(pair[0], pair[1], in_weight, mid_weight, out_weight), (current, embeds))
            drift = (coef_one - 1.0)[:, None, None] * current + coef_two[:, None, None] * noise
            totals = jnp.cumsum(drift, axis=0)
            prefix = jnp.concatenate([jnp.zeros_like(drift[:1]), totals[:-1]], axis=0)
            updated = current[0:1] + prefix
            updated = jnp.concatenate([current[0:1], updated[1:]], axis=0)
            sweep_rows.append(lax.optimization_barrier(jnp.mean((updated - current) ** 2, axis=(1, 2))))
            current = updated
        error_rows.append(jnp.stack(sweep_rows))
        advance = advances[round_no]
        source = jnp.minimum(places + advance, window - 1).astype(jnp.int32)
        current = current[source]
        window_start = window_start + advance
    return (current, jnp.stack(error_rows))
```

```python
import functools
import math

import jax
import jax.numpy as jnp
import numpy as np
from jax import lax
from jax.experimental import pallas as pl
from jax.experimental.pallas import tpu as pltpu
from jax.sharding import PartitionSpec as P

TSTEPS = 1000
ITERS = 4
ROUNDS = 2
LANES = 128
BASE = 32
XROWS = 16
TILE = 256
LAG_MIXED = 1
LAG_NOISE = 3
VECTOR_ROWS = 112


def alpha_table():
    levels = np.arange(TSTEPS, dtype=np.float64)
    low = math.sqrt(0.00085)
    high = math.sqrt(0.012)
    betas = (low + (high - low) * levels / (TSTEPS - 1)) ** 2
    return np.exp(np.cumsum(np.log1p(-betas))).astype(np.float32)


def trig_tables(width):
    half = width // 2
    freqs = np.exp(-math.log(10000.0) * np.arange(half, dtype=np.float64) / half)[:, None]
    digits = np.arange(BASE, dtype=np.float64)[None]
    high, low = freqs * digits * BASE, freqs * digits
    coarse = np.concatenate([np.cos(high), np.sin(high)]).astype(np.float32)
    fine = np.concatenate([np.cos(low), np.sin(low)]).astype(np.float32)
    return np.concatenate([coarse, fine])


def round_up(value, unit):
    return -(-value // unit) * unit


def kernel(
    n, pix, width, depth, direct, vector_rows, fused,
    states_hbm, sched_ref, adv_ref, alpha_ref, inw_hbm, outw_hbm, timew_hbm, midw_hbm, trig_hbm,
    out_ref, err_ref,
    states_ref, inw_ref, outw_ref, timew, midw, trig, xin, xs, fin, errs, elines, erecv, lhs, mid, outs, outw, inw, coef_one, coef_two,
    in_table, time_table, linear_in, linear_time,
    local, in_send, in_recv, out_send, out_recv, err_send, err_recv,
):
    lat = outw_ref.shape[0]
    ch = midw.shape[0]
    me = lax.axis_index("steps")
    span = ROUNDS * n
    f32, bf16 = jnp.float32, jnp.bfloat16

    def peer(hop):
        return lax.rem(me + hop, n)

    def source(d):
        if direct:
            return states_ref.at[0, :, pl.ds(pl.multiple_of(d * pix, LANES), pix)]
        return states_ref.at[d]

    def target(d):
        if direct:
            return out_ref.at[0, :, pl.ds(pl.multiple_of(d * pix, LANES), pix)]
        return out_ref.at[d]

    def in_copy(d, slot):
        return pltpu.make_async_remote_copy(
            src_ref=source(d), dst_ref=xin.at[slot], send_sem=in_send.at[d], recv_sem=in_recv.at[slot],
            device_id={"steps": d}, device_id_type=pl.DeviceIdType.MESH)

    def out_copy(d, slot):
        return pltpu.make_async_remote_copy(
            src_ref=fin.at[d], dst_ref=target(slot), send_sem=out_send.at[d], recv_sem=out_recv.at[slot],
            device_id={"steps": d}, device_id_type=pl.DeviceIdType.MESH)

    def err_copy(d, slot):
        return pltpu.make_async_remote_copy(
            src_ref=elines.at[d], dst_ref=erecv.at[slot], send_sem=err_send.at[d], recv_sem=err_recv.at[slot],
            device_id={"steps": d}, device_id_type=pl.DeviceIdType.MESH)

    def each_peer(act):
        if n <= 16:
            for hop in range(1, n):
                act(peer(hop))
        else:
            @pl.loop(1, n)
            def _(hop):
                act(peer(hop))

    loads = [
        pltpu.make_async_copy(source_ref, held, local.at[j])
        for j, (source_ref, held) in enumerate((
            (states_hbm, states_ref), (trig_hbm, trig), (timew_hbm, timew), (midw_hbm, midw),
            (inw_hbm, inw_ref), (outw_hbm, outw_ref)))
    ]
    for load in loads:
        load.start()
    barrier = pltpu.get_barrier_semaphore()
    each_peer(lambda d: pl.semaphore_signal(
        barrier, inc=1, device_id={"steps": d}, device_id_type=pl.DeviceIdType.MESH))

    lane = lax.broadcasted_iota(jnp.int32, (1, depth), 1) - XROWS
    member = jnp.where((lane >= 0) & (lane < 3 * span), lax.rem(jnp.maximum(lane, 0), span), -1)
    advance_one = adv_ref[0]

    def coefficients(m, stamps):
        place = jnp.where(m >= n, advance_one + m - n, m)
        now, after = sched_ref[place], sched_ref[place + 1]
        a_now = jnp.full((8, LANES), alpha_ref[now], f32)
        a_after = jnp.full((8, LANES), alpha_ref[after], f32)
        one = jnp.sqrt(a_after / a_now)
        two = jnp.sqrt(1.0 - a_after) - one * jnp.sqrt(1.0 - a_now)
        coef_one[m] = one - 1.0
        coef_two[m] = two
        return jnp.where(member == m, now, stamps)

    stamps = lax.fori_loop(0, span, coefficients, jnp.zeros((1, depth), jnp.int32), unroll=4)

    loads[0].wait()
    pl.semaphore_wait(barrier, n - 1)
    each_peer(lambda d: in_copy(d, me).start())

    digit = lax.broadcasted_iota(jnp.int32, (BASE, depth), 0)
    hot_high = (digit == lax.shift_right_logical(stamps, 5)).astype(f32)
    hot_low = (digit == lax.bitwise_and(stamps, BASE - 1)).astype(f32)
    exact = lax.Precision.HIGHEST
    for load in loads[1:]:
        load.wait()
    high = jnp.dot(trig[0:ch], hot_high, precision=exact, preferred_element_type=f32)
    low = jnp.dot(trig[ch:], hot_low, precision=exact, preferred_element_type=f32)
    half = ch // 2
    cos_h, sin_h, cos_l, sin_l = high[:half], high[half:], low[:half], low[half:]
    feats = jnp.concatenate([cos_h * cos_l - sin_h * sin_l, sin_h * cos_l + cos_h * sin_l], axis=0)
    embed = 0.5 * jnp.dot(timew[...], feats, precision=exact, preferred_element_type=f32)
    inw[...] = jnp.zeros_like(inw)
    inw[0:lat, :] = inw_ref[...].astype(f32) * 0.5
    unit = (lax.broadcasted_iota(jnp.int32, (8, depth), 0) == lane + XROWS).astype(f32)
    spread = lax.dot_general(
        inw[...], unit, (((0,), (0,)), ((), ())), precision=exact, preferred_element_type=f32)
    top = embed.astype(bf16).astype(f32)
    rest = embed - top
    middle = rest.astype(bf16).astype(f32)
    bottom = (rest - middle).astype(bf16).astype(f32)
    part = jnp.where(lane < span, top, jnp.where(lane < 2 * span, middle, bottom))
    part = jnp.where(member >= 0, part, 0.0)
    left = spread + part
    matrix_rows = ch - vector_rows
    outw[...] = jnp.zeros_like(outw)
    outw[0:lat, :] = outw_ref[...].astype(f32)
    half_mid = (midw[...].astype(f32) * 0.5).astype(bf16)
    padded_out = jnp.concatenate([outw[...], jnp.zeros_like(outw[...])], axis=0).astype(bf16)
    narrow = lambda rows, lanes: jnp.zeros((rows, lanes), bf16)
    cuts_one = (0, TILE - LANES // 2, ch)
    cuts_two = (0, LANES // 2, TILE - (ch - cuts_one[1]) + LANES // 2, ch)
    if fused:
        for part in range(2):
            one = half_mid[:, cuts_one[part]:cuts_one[part + 1]]
            two = padded_out[:, cuts_two[part]:cuts_two[part + 1]]
            mid[part, 0:ch, :] = jnp.concatenate([one, narrow(ch, two.shape[1])], axis=1)
            mid[part, ch:, :] = jnp.concatenate([narrow(16, one.shape[1]), two], axis=1)
        lhs[0:16, 0:LANES] = padded_out[:, cuts_two[2]:]
        lhs[0:16, LANES:] = narrow(16, depth)
        lhs[16:, 0:LANES] = narrow(matrix_rows, LANES)
        lhs[16:, LANES:] = left[0:matrix_rows].astype(bf16)
    else:
        mid[...] = half_mid
        outs[...] = padded_out
        lhs[...] = left[0:matrix_rows].astype(bf16)
    whole = spread + jnp.where(member >= 0, embed, 0.0)
    linear = 2.0 * jnp.dot(outw[...], whole, precision=exact, preferred_element_type=f32)
    for l in range(lat):
        linear_in[l] = jnp.broadcast_to(linear[:, l:l + 1], (8, LANES))
        if vector_rows:
            in_table[l] = jnp.broadcast_to(whole[matrix_rows:, l:l + 1], (vector_rows, LANES))
    for m in range(span):
        at = XROWS + m
        linear_time[m] = jnp.broadcast_to(linear[:, at:at + 1], (8, LANES))
        if vector_rows:
            time_table[m] = jnp.broadcast_to(whole[matrix_rows:, at:at + 1], (vector_rows, LANES))

    xs[0] = jnp.zeros_like(xs[0])
    errs[...] = jnp.zeros_like(errs)
    if direct:
        xs[0, me, 0:lat, :] = states_ref[0, :, pl.ds(pl.multiple_of(me * pix, LANES), pix)]
    else:
        xs[0, me, 0:lat, :] = states_ref[me]

    def arrived(d):
        in_copy(d, d).wait_recv()
        xs[0, d, 0:lat, :] = xin[d]

    each_peer(arrived)

    hot_row = lax.broadcasted_iota(jnp.int32, (depth - XROWS, LANES), 0)
    hot_member = jnp.where(hot_row < 3 * span, lax.rem(hot_row, span), -1)
    wide = lambda tile: jnp.concatenate([tile] * (width // LANES), axis=1) if width > LANES else tile

    def swish(half):
        return half + half * jnp.tanh(half)

    join = lambda parts: parts[0] if len(parts) == 1 else jnp.concatenate(parts, axis=1)
    tiles = [slice(start, start + LANES) for start in range(0, width, LANES)]

    def affine(base, slopes, x, tile):
        total = base
        for l in range(lat):
            total = total + slopes[l] * x[l:l + 1, tile]
        return total

    def column(x, m):
        hot = wide((hot_member == m).astype(f32).astype(bf16))
        padded = jnp.concatenate([x, jnp.zeros((XROWS - 8, width), f32)], axis=0).astype(bf16)
        return jnp.concatenate([padded, hot], axis=0)

    def vector_part(x, m):
        rounded = x.astype(bf16).astype(f32)
        tail = join([affine(linear_time[m], linear_in, rounded, tile) for tile in tiles])
        if not vector_rows:
            return tail, None
        return tail, join([swish(affine(time_table[m], in_table, rounded, tile).astype(bf16)) for tile in tiles])

    def product(weights, values):
        return jnp.dot(weights, values, preferred_element_type=f32)

    def note_error(row, k, change):
        square = change * change
        if pix < width:
            square = jnp.where(lax.broadcasted_iota(jnp.int32, square.shape, 1) < pix, square, 0.0)
        total = square[:, 0:LANES]
        for start in range(LANES, width, LANES):
            total = total + square[:, start:start + LANES]
        errs[k, pl.ds(row, 1), :] = jnp.sum(total, axis=0, keepdims=True)

    def moved(r, m_at, old, noise):
        return wide(coef_one[m_at]) * old + wide(coef_two[m_at]) * noise

    def flat_round(r):
        todo = [(i, k) for i in range(ITERS) for k in range(i, n - 1)]
        groups = [todo[j:j + 2] for j in range(0, len(todo), 2)]
        count = len(groups)
        tails, hidden, late, running = {}, {}, {}, {}

        def finish(i, k, noise):
            row = r * ITERS + i
            old = xs[i, k]
            if k == i:
                running[i] = old
                xs[ITERS, k] = old
            running[i] = running[i] + moved(r, r * n + k, old, noise)
            note_error(row, k + 1, running[i] - xs[i, k + 1])
            xs[i + 1, k + 1] = running[i]

        def pad(values, lanes):
            return values if values.shape[1] == lanes else jnp.concatenate(
                [values, jnp.zeros((values.shape[0], lanes - values.shape[1]), bf16)], axis=1)

        for step in range(count + LAG_NOISE):
            new, second, third = step, step - LAG_MIXED, step - LAG_NOISE
            has_new, has_second, has_third = new < count, 0 <= second < count, 0 <= third < count
            sizes = [len(groups[g]) * width for g, there in ((new, has_new), (second, has_second), (third, has_third)) if there]
            lanes = max(sizes)
            noise = mixed = None
            if has_new:
                now, extras, ends = [], [], []
                for i, k in groups[new]:
                    x = xs[i, k]
                    now.append(column(x, r * n + k))
                    tail, extra = vector_part(x, r * n + k)
                    ends.append(tail)
                    extras.append(extra)
                tails[new] = ends
                new_rows = pad(join(now), lanes)
            else:
                new_rows = jnp.zeros((depth, lanes), bf16)
            old_rows = pad(late[third], lanes) if has_third else jnp.zeros((ch, lanes), bf16)
            mid_rows = pad(hidden[second], lanes) if has_second else jnp.zeros((ch, lanes), bf16)
            if has_new or has_third:
                begin = 0 if has_third else 16
                end = lhs.shape[0] if has_new else 16
                both = product(lhs[begin:end], jnp.concatenate([old_rows[cuts_two[2]:], new_rows], axis=0))
                if has_new:
                    hid = swish(both[16 - begin:, 0:len(groups[new]) * width].astype(bf16))
                    hidden[new] = jnp.concatenate([hid, join(extras)], axis=0) if vector_rows else hid
                if has_third:
                    noise = both[0:8]
            if has_second or has_third:
                begin = 0 if has_second else ch
                end = ch + 16 if has_third else ch
                for part in range(2):
                    values = jnp.concatenate([
                        mid_rows[cuts_one[part]:cuts_one[part + 1]], old_rows[cuts_two[part]:cuts_two[part + 1]]], axis=0)
                    both = product(mid[part, begin:end], values)
                    if has_second:
                        mixed = both[0:ch] if mixed is None else mixed + both[0:ch]
                    if has_third:
                        noise = noise + both[ch - begin:ch - begin + 8]
            if has_second:
                late[second] = swish(mixed[:, 0:len(groups[second]) * width].astype(bf16))
                del hidden[second]
            if has_third:
                for j, (i, k) in enumerate(groups[third]):
                    finish(i, k, tails[third][j] + noise[:, j * width:(j + 1) * width])
                del late[third]

    def rolled_round(r):
        for i in range(ITERS):
            row = r * ITERS + i

            def body(k, running):
                old = xs[0, k]
                tail, _ = vector_part(old, r * n + k)
                hid = swish(product(lhs[...], column(old, r * n + k)).astype(bf16))
                noise = tail + product(outs[...], swish(product(mid[...], hid).astype(bf16)))[0:8]
                note_error(row, k, running - old)
                xs[0, k] = running
                return running + moved(r, r * n + k, old, noise)

            running = lax.fori_loop(i, n - 1, body, xs[0, i])
            note_error(row, n - 1, running - xs[0, n - 1])
            xs[0, n - 1] = running

    def one_round(r, carry):
        advance = adv_ref[r]
        if fused:
            flat_round(r)
            for k in range(n):
                xs[0, k] = xs[ITERS, jnp.minimum(k + advance, n - 1)]
        else:
            rolled_round(r)

            def shift(k, carry):
                xs[0, k] = xs[0, jnp.minimum(k + advance, n - 1)]
                return carry

            lax.fori_loop(0, n, shift, 0, unroll=4)
        return carry

    lax.fori_loop(0, ROUNDS, one_round, 0)
    for k in range(n):
        fin[k] = xs[0, k, 0:lat, :]
    each_peer(lambda d: out_copy(d, me).start())
    cells = (ROUNDS * ITERS, LANES)
    diagonal = lax.broadcasted_iota(jnp.int32, cells, 0) == lax.broadcasted_iota(jnp.int32, cells, 1)
    for k in range(n):
        total = jnp.sum(errs[k], axis=1, keepdims=True)
        elines[k] = jnp.sum(jnp.where(diagonal, total, 0.0), axis=0, keepdims=True)
    each_peer(lambda d: err_copy(d, me).start())
    if direct:
        out_ref[0, :, pl.ds(pl.multiple_of(me * pix, LANES), pix)] = fin[me]
    else:
        out_ref[me] = fin[me]
    erecv[me] = elines[me]
    each_peer(lambda d: err_copy(d, d).wait_recv())
    sums = lax.fori_loop(0, n, lambda k, total: total + erecv[k], jnp.zeros((1, LANES), f32), unroll=4)
    means = jnp.sum(jnp.where(diagonal, sums, 0.0), axis=1, keepdims=True) * (1.0 / (lat * n * pix))
    for r in range(ROUNDS):
        err_ref[r] = means[r * ITERS:(r + 1) * ITERS]
    each_peer(lambda d: out_copy(d, d).wait_recv())
    each_peer(lambda d: in_copy(d, me).wait_send())
    each_peer(lambda d: out_copy(d, me).wait_send())
    each_peer(lambda d: err_copy(d, me).wait_send())


def shards(states, t_sched, advances, in_weight, time_weight, mid_weight, out_weight):
    n = lax.axis_size("steps")
    _, lat, rows = states.shape
    ch = mid_weight.shape[0]
    pix = rows // n
    direct = pix % LANES == 0
    width = round_up(pix, LANES)
    depth = round_up(XROWS + 3 * ROUNDS * n, LANES)
    fused = (
        n <= 16 and width == TILE and ch == TILE + LANES // 2 and depth == LANES
        and (n - ITERS + 1) // 2 > LAG_NOISE and VECTOR_ROWS < ch)
    vector_rows = VECTOR_ROWS if fused else 0
    if direct:
        sent = states
        out_shape = states.shape
    else:
        sent = jnp.pad(states.reshape(lat, n, pix).transpose(1, 0, 2), ((0, 0), (0, 0), (0, width - pix)))
        out_shape = sent.shape
    vmem = pl.BlockSpec(memory_space=pltpu.VMEM)
    smem = pl.BlockSpec(memory_space=pltpu.SMEM)
    hbm = pl.BlockSpec(memory_space=pltpu.HBM)
    f32, bf16 = jnp.float32, jnp.bfloat16
    final, errors = pl.pallas_call(
        functools.partial(kernel, n, pix, width, depth, direct, vector_rows, fused),
        out_shape=(jax.ShapeDtypeStruct(out_shape, f32), jax.ShapeDtypeStruct((ROUNDS, ITERS, 1), f32)),
        in_specs=[hbm, smem, smem, smem, hbm, hbm, hbm, hbm, hbm],
        out_specs=(vmem, vmem),
        scratch_shapes=[
            pltpu.VMEM(sent.shape, f32),
            pltpu.VMEM((lat, ch), bf16),
            pltpu.VMEM((lat, ch), bf16),
            pltpu.VMEM((ch, ch), f32),
            pltpu.VMEM((ch, ch), bf16),
            pltpu.VMEM((2 * ch, BASE), f32),
            pltpu.VMEM((n, lat, width), f32),
            pltpu.VMEM((ITERS + 1, n, 8, width), f32),
            pltpu.VMEM((n, lat, width), f32),
            pltpu.VMEM((n, ROUNDS * ITERS, LANES), f32),
            pltpu.VMEM((n, 1, LANES), f32),
            pltpu.VMEM((n, 1, LANES), f32),
            pltpu.VMEM((16 + ch - vector_rows, LANES + depth) if fused else (ch, depth), bf16),
            pltpu.VMEM((2, ch + 16, TILE) if fused else (ch, ch), bf16),
            pltpu.VMEM((16, ch), bf16),
            pltpu.VMEM((8, ch), f32),
            pltpu.VMEM((8, ch), f32),
            pltpu.VMEM((ROUNDS * n, 8, LANES), f32),
            pltpu.VMEM((ROUNDS * n, 8, LANES), f32),
            pltpu.VMEM((lat, max(vector_rows, 8), LANES), f32),
            pltpu.VMEM((ROUNDS * n, max(vector_rows, 8), LANES), f32),
            pltpu.VMEM((lat, 8, LANES), f32),
            pltpu.VMEM((ROUNDS * n, 8, LANES), f32),
            pltpu.SemaphoreType.DMA((6,)),
        ] + [pltpu.SemaphoreType.DMA((n,))] * 6,
        compiler_params=pltpu.CompilerParams(
            collective_id=0, has_side_effects=True, vmem_limit_bytes=67043328),
        name="picard",
    )(sent, t_sched, advances, jnp.asarray(alpha_table()), in_weight.T, out_weight, time_weight, mid_weight,
      jnp.asarray(trig_tables(time_weight.shape[1])))
    if not direct:
        final = final[:, :, :pix].transpose(1, 0, 2).reshape(states.shape)
    return final, errors


def solution(mesh):
    in_specs = (P(("groups", "steps"), None, None), P("groups"), P("groups"), P(), P(), P(), P())
    out_specs = (P(("groups", "steps"), None, None), P("groups", None, "steps"))
    return jax.shard_map(shards, mesh=mesh, in_specs=in_specs, out_specs=out_specs, check_vma=False)
```

```python
import functools
import math

import jax
import jax.numpy as jnp
import numpy as np
from jax import lax
from jax.experimental import pallas as pl
from jax.experimental.pallas import tpu as pltpu
from jax.sharding import PartitionSpec as P

TSTEPS = 1000
ITERS = 4
ROUNDS = 2
LANES = 128
BASE = 32
XROWS = 16
TILE = 256
LAG_MIXED = 1
LAG_NOISE = 3
VMEM_BYTES = 40 << 20
VECTOR_ROWS = 112


def alpha_table():
    levels = np.arange(TSTEPS, dtype=np.float64)
    low = math.sqrt(0.00085)
    high = math.sqrt(0.012)
    betas = (low + (high - low) * levels / (TSTEPS - 1)) ** 2
    return np.exp(np.cumsum(np.log1p(-betas))).astype(np.float32)


def trig_tables(width):
    half = width // 2
    freqs = np.exp(-math.log(10000.0) * np.arange(half, dtype=np.float64) / half)[:, None]
    digits = np.arange(BASE, dtype=np.float64)[None]
    high, low = freqs * digits * BASE, freqs * digits
    coarse = np.concatenate([np.cos(high), np.sin(high)]).astype(np.float32)
    fine = np.concatenate([np.cos(low), np.sin(low)]).astype(np.float32)
    return np.concatenate([coarse, fine])


def round_up(value, unit):
    return -(-value // unit) * unit


def kernel(
    n, pix, width, depth, direct, vector_rows, fused,
    states_hbm, sched_hbm, adv_hbm, alpha_hbm, inw_hbm, outw_hbm, timew_hbm, midw_hbm, trig_hbm,
    out_ref, err_ref,
    sched_ref, adv_ref, alpha_ref, states_ref, inw_ref, outw_ref, timew, midw, trig, xin, xs, fin, errs, elines, erecv, lhs, mid, outs, outw, inw, coef_one, coef_two,
    in_table, time_table, linear_in, linear_time,
    local, in_send, in_recv, out_send, out_recv, err_send, err_recv,
):
    lat = outw_ref.shape[0]
    ch = midw.shape[0]
    me = lax.axis_index("steps")
    span = ROUNDS * n
    f32, bf16 = jnp.float32, jnp.bfloat16

    def peer(hop):
        return lax.rem(me + hop, n)

    def source(d):
        if direct:
            return states_ref.at[0, :, pl.ds(pl.multiple_of(d * pix, LANES), pix)]
        return states_ref.at[d]

    def target(d):
        if direct:
            return out_ref.at[0, :, pl.ds(pl.multiple_of(d * pix, LANES), pix)]
        return out_ref.at[d]

    def in_copy(d, slot):
        return pltpu.make_async_remote_copy(
            src_ref=source(d), dst_ref=xin.at[slot], send_sem=in_send.at[d], recv_sem=in_recv.at[slot],
            device_id={"steps": d}, device_id_type=pl.DeviceIdType.MESH)

    def out_copy(d, slot):
        return pltpu.make_async_remote_copy(
            src_ref=fin.at[d], dst_ref=target(slot), send_sem=out_send.at[d], recv_sem=out_recv.at[slot],
            device_id={"steps": d}, device_id_type=pl.DeviceIdType.MESH)

    def err_copy(d, slot):
        return pltpu.make_async_remote_copy(
            src_ref=elines.at[d], dst_ref=erecv.at[slot], send_sem=err_send.at[d], recv_sem=err_recv.at[slot],
            device_id={"steps": d}, device_id_type=pl.DeviceIdType.MESH)

    def each_peer(act):
        if n <= 16:
            for hop in range(1, n):
                act(peer(hop))
        else:
            @pl.loop(1, n)
            def _(hop):
                act(peer(hop))

    barrier = pltpu.get_barrier_semaphore()
    each_peer(lambda d: pl.semaphore_signal(
        barrier, inc=1, device_id={"steps": d}, device_id_type=pl.DeviceIdType.MESH))
    loads = [
        pltpu.make_async_copy(source_ref, held, local.at[j])
        for j, (source_ref, held) in enumerate((
            (states_hbm, states_ref), (sched_hbm, sched_ref), (adv_hbm, adv_ref), (alpha_hbm, alpha_ref),
            (trig_hbm, trig), (timew_hbm, timew), (midw_hbm, midw), (inw_hbm, inw_ref), (outw_hbm, outw_ref)))
    ]
    for load in loads:
        load.start()
    loads[0].wait()
    pl.semaphore_wait(barrier, n - 1)
    each_peer(lambda d: in_copy(d, me).start())

    for load in loads[1:4]:
        load.wait()
    lane = lax.broadcasted_iota(jnp.int32, (1, depth), 1) - XROWS
    member = jnp.where((lane >= 0) & (lane < 3 * span), lax.rem(jnp.maximum(lane, 0), span), -1)
    advance_one = adv_ref[0]

    def coefficients(m, stamps):
        place = jnp.where(m >= n, advance_one + m - n, m)
        now, after = sched_ref[place], sched_ref[place + 1]
        a_now = jnp.full((8, LANES), alpha_ref[now], f32)
        a_after = jnp.full((8, LANES), alpha_ref[after], f32)
        one = jnp.sqrt(a_after / a_now)
        two = jnp.sqrt(1.0 - a_after) - one * jnp.sqrt(1.0 - a_now)
        coef_one[m] = one - 1.0
        coef_two[m] = two
        return jnp.where(member == m, now, stamps)

    stamps = lax.fori_loop(0, span, coefficients, jnp.zeros((1, depth), jnp.int32), unroll=8)

    digit = lax.broadcasted_iota(jnp.int32, (BASE, depth), 0)
    hot_high = (digit == lax.shift_right_logical(stamps, 5)).astype(f32)
    hot_low = (digit == lax.bitwise_and(stamps, BASE - 1)).astype(f32)
    exact = lax.Precision.HIGHEST
    for load in loads[4:]:
        load.wait()
    high = jnp.dot(trig[0:ch], hot_high, precision=exact, preferred_element_type=f32)
    low = jnp.dot(trig[ch:], hot_low, precision=exact, preferred_element_type=f32)
    half = ch // 2
    cos_h, sin_h, cos_l, sin_l = high[:half], high[half:], low[:half], low[half:]
    feats = jnp.concatenate([cos_h * cos_l - sin_h * sin_l, sin_h * cos_l + cos_h * sin_l], axis=0)
    embed = 0.5 * jnp.dot(timew[...], feats, precision=exact, preferred_element_type=f32)
    inw[...] = jnp.zeros_like(inw)
    inw[0:lat, :] = inw_ref[...].astype(f32) * 0.5
    unit = (lax.broadcasted_iota(jnp.int32, (8, depth), 0) == lane + XROWS).astype(f32)
    spread = lax.dot_general(
        inw[...], unit, (((0,), (0,)), ((), ())), precision=exact, preferred_element_type=f32)
    top = embed.astype(bf16).astype(f32)
    rest = embed - top
    middle = rest.astype(bf16).astype(f32)
    bottom = (rest - middle).astype(bf16).astype(f32)
    part = jnp.where(lane < span, top, jnp.where(lane < 2 * span, middle, bottom))
    part = jnp.where(member >= 0, part, 0.0)
    left = spread + part
    matrix_rows = ch - vector_rows
    outw[...] = jnp.zeros_like(outw)
    outw[0:lat, :] = outw_ref[...].astype(f32)
    half_mid = (midw[...].astype(f32) * 0.5).astype(bf16)
    padded_out = jnp.concatenate([outw[...], jnp.zeros_like(outw[...])], axis=0).astype(bf16)
    narrow = lambda rows, lanes: jnp.zeros((rows, lanes), bf16)
    cuts_one = (0, TILE - LANES // 2, ch)
    cuts_two = (0, LANES // 2, TILE - (ch - cuts_one[1]) + LANES // 2, ch)
    if fused:
        for part in range(2):
            one = half_mid[:, cuts_one[part]:cuts_one[part + 1]]
            two = padded_out[:, cuts_two[part]:cuts_two[part + 1]]
            mid[part, 0:ch, :] = jnp.concatenate([one, narrow(ch, two.shape[1])], axis=1)
            mid[part, ch:, :] = jnp.concatenate([narrow(16, one.shape[1]), two], axis=1)
        lhs[0:16, 0:LANES] = padded_out[:, cuts_two[2]:]
        lhs[0:16, LANES:] = narrow(16, depth)
        lhs[16:, 0:LANES] = narrow(matrix_rows, LANES)
        lhs[16:, LANES:] = left[0:matrix_rows].astype(bf16)
    else:
        mid[...] = half_mid
        outs[...] = padded_out
        lhs[...] = left[0:matrix_rows].astype(bf16)
    whole = spread + jnp.where(member >= 0, embed, 0.0)
    linear = 2.0 * jnp.dot(outw[...], whole, precision=exact, preferred_element_type=f32)
    for l in range(lat):
        linear_in[l] = jnp.broadcast_to(linear[:, l:l + 1], (8, LANES))
        if vector_rows:
            in_table[l] = jnp.broadcast_to(whole[matrix_rows:, l:l + 1], (vector_rows, LANES))
    for m in range(span):
        at = XROWS + m
        linear_time[m] = jnp.broadcast_to(linear[:, at:at + 1], (8, LANES))
        if vector_rows:
            time_table[m] = jnp.broadcast_to(whole[matrix_rows:, at:at + 1], (vector_rows, LANES))

    xs[0] = jnp.zeros_like(xs[0])
    errs[...] = jnp.zeros_like(errs)
    if direct:
        xs[0, me, 0:lat, :] = states_ref[0, :, pl.ds(pl.multiple_of(me * pix, LANES), pix)]
    else:
        xs[0, me, 0:lat, :] = states_ref[me]

    def arrived(d):
        in_copy(d, d).wait_recv()
        xs[0, d, 0:lat, :] = xin[d]

    each_peer(arrived)

    hot_row = lax.broadcasted_iota(jnp.int32, (depth - XROWS, LANES), 0)
    hot_member = jnp.where(hot_row < 3 * span, lax.rem(hot_row, span), -1)
    wide = lambda tile: jnp.concatenate([tile] * (width // LANES), axis=1) if width > LANES else tile

    def swish(half):
        return half + half * jnp.tanh(half)

    join = lambda parts: parts[0] if len(parts) == 1 else jnp.concatenate(parts, axis=1)
    tiles = [slice(start, start + LANES) for start in range(0, width, LANES)]

    def affine(base, slopes, x, tile):
        total = base
        for l in range(lat):
            total = total + slopes[l] * x[l:l + 1, tile]
        return total

    def column(x, m):
        hot = wide((hot_member == m).astype(f32).astype(bf16))
        padded = jnp.concatenate([x, jnp.zeros((XROWS - 8, width), f32)], axis=0).astype(bf16)
        return jnp.concatenate([padded, hot], axis=0)

    def vector_part(x, m):
        rounded = x.astype(bf16).astype(f32)
        tail = join([affine(linear_time[m], linear_in, rounded, tile) for tile in tiles])
        if not vector_rows:
            return tail, None
        return tail, join([swish(affine(time_table[m], in_table, rounded, tile).astype(bf16)) for tile in tiles])

    def product(weights, values):
        return jnp.dot(weights, values, preferred_element_type=f32)

    def note_error(row, k, change):
        square = change * change
        if pix < width:
            square = jnp.where(lax.broadcasted_iota(jnp.int32, square.shape, 1) < pix, square, 0.0)
        total = square[:, 0:LANES]
        for start in range(LANES, width, LANES):
            total = total + square[:, start:start + LANES]
        errs[k, pl.ds(row, 1), :] = jnp.sum(total, axis=0, keepdims=True)

    def moved(r, m_at, old, noise):
        return wide(coef_one[m_at]) * old + wide(coef_two[m_at]) * noise

    def flat_round(r):
        todo = [(i, k) for i in range(ITERS) for k in range(i, n - 1)]
        groups = [todo[j:j + 2] for j in range(0, len(todo), 2)]
        count = len(groups)
        tails, hidden, late, running = {}, {}, {}, {}

        def finish(i, k, noise):
            row = r * ITERS + i
            old = xs[i, k]
            if k == i:
                running[i] = old
                xs[ITERS, k] = old
            running[i] = running[i] + moved(r, r * n + k, old, noise)
            note_error(row, k + 1, running[i] - xs[i, k + 1])
            xs[i + 1, k + 1] = running[i]

        def pad(values, lanes):
            return values if values.shape[1] == lanes else jnp.concatenate(
                [values, jnp.zeros((values.shape[0], lanes - values.shape[1]), bf16)], axis=1)

        for step in range(count + LAG_NOISE):
            new, second, third = step, step - LAG_MIXED, step - LAG_NOISE
            has_new, has_second, has_third = new < count, 0 <= second < count, 0 <= third < count
            sizes = [len(groups[g]) * width for g, there in ((new, has_new), (second, has_second), (third, has_third)) if there]
            lanes = max(sizes)
            noise = mixed = None
            if has_new:
                now, extras, ends = [], [], []
                for i, k in groups[new]:
                    x = xs[i, k]
                    now.append(column(x, r * n + k))
                    tail, extra = vector_part(x, r * n + k)
                    ends.append(tail)
                    extras.append(extra)
                tails[new] = ends
                new_rows = pad(join(now), lanes)
            else:
                new_rows = jnp.zeros((depth, lanes), bf16)
            old_rows = pad(late[third], lanes) if has_third else jnp.zeros((ch, lanes), bf16)
            mid_rows = pad(hidden[second], lanes) if has_second else jnp.zeros((ch, lanes), bf16)
            if has_new or has_third:
                begin = 0 if has_third else 16
                end = lhs.shape[0] if has_new else 16
                both = product(lhs[begin:end], jnp.concatenate([old_rows[cuts_two[2]:], new_rows], axis=0))
                if has_new:
                    hid = swish(both[16 - begin:, 0:len(groups[new]) * width].astype(bf16))
                    hidden[new] = jnp.concatenate([hid, join(extras)], axis=0) if vector_rows else hid
                if has_third:
                    noise = both[0:8]
            if has_second or has_third:
                begin = 0 if has_second else ch
                end = ch + 16 if has_third else ch
                for part in range(2):
                    values = jnp.concatenate([
                        mid_rows[cuts_one[part]:cuts_one[part + 1]], old_rows[cuts_two[part]:cuts_two[part + 1]]], axis=0)
                    both = product(mid[part, begin:end], values)
                    if has_second:
                        mixed = both[0:ch] if mixed is None else mixed + both[0:ch]
                    if has_third:
                        noise = noise + both[ch - begin:ch - begin + 8]
            if has_second:
                late[second] = swish(mixed[:, 0:len(groups[second]) * width].astype(bf16))
                del hidden[second]
            if has_third:
                for j, (i, k) in enumerate(groups[third]):
                    finish(i, k, tails[third][j] + noise[:, j * width:(j + 1) * width])
                del late[third]

    def rolled_round(r):
        for i in range(ITERS):
            row = r * ITERS + i

            def body(k, running):
                old = xs[0, k]
                tail, _ = vector_part(old, r * n + k)
                hid = swish(product(lhs[...], column(old, r * n + k)).astype(bf16))
                noise = tail + product(outs[...], swish(product(mid[...], hid).astype(bf16)))[0:8]
                note_error(row, k, running - old)
                xs[0, k] = running
                return running + moved(r, r * n + k, old, noise)

            running = lax.fori_loop(i, n - 1, body, xs[0, i])
            note_error(row, n - 1, running - xs[0, n - 1])
            xs[0, n - 1] = running

    def one_round(r, carry):
        advance = adv_ref[r]
        if fused:
            flat_round(r)
            for k in range(n):
                xs[0, k] = xs[ITERS, jnp.minimum(k + advance, n - 1)]
        else:
            rolled_round(r)

            def shift(k, carry):
                xs[0, k] = xs[0, jnp.minimum(k + advance, n - 1)]
                return carry

            lax.fori_loop(0, n, shift, 0, unroll=4)
        return carry

    lax.fori_loop(0, ROUNDS, one_round, 0)
    for k in range(n):
        fin[k] = xs[0, k, 0:lat, :]
    each_peer(lambda d: out_copy(d, me).start())
    cells = (ROUNDS * ITERS, LANES)
    diagonal = lax.broadcasted_iota(jnp.int32, cells, 0) == lax.broadcasted_iota(jnp.int32, cells, 1)
    for k in range(n):
        total = jnp.sum(errs[k], axis=1, keepdims=True)
        elines[k] = jnp.sum(jnp.where(diagonal, total, 0.0), axis=0, keepdims=True)
    each_peer(lambda d: err_copy(d, me).start())
    if direct:
        out_ref[0, :, pl.ds(pl.multiple_of(me * pix, LANES), pix)] = fin[me]
    else:
        out_ref[me] = fin[me]
    erecv[me] = elines[me]
    each_peer(lambda d: err_copy(d, d).wait_recv())
    sums = lax.fori_loop(0, n, lambda k, total: total + erecv[k], jnp.zeros((1, LANES), f32), unroll=4)
    means = sums * (1.0 / (lat * n * pix))
    for r in range(ROUNDS):
        err_ref[r] = means[:, r * ITERS:(r + 1) * ITERS]
    each_peer(lambda d: out_copy(d, d).wait_recv())
    each_peer(lambda d: in_copy(d, me).wait_send())
    each_peer(lambda d: out_copy(d, me).wait_send())
    each_peer(lambda d: err_copy(d, me).wait_send())


def closing(final_ref, errors_ref, final_out, errors_out, sems):
    copies = [
        pltpu.make_async_copy(final_ref, final_out, sems.at[0]),
        pltpu.make_async_copy(errors_ref, errors_out, sems.at[1]),
    ]
    for copy in copies:
        copy.start()
    for copy in copies:
        copy.wait()


def shards(states, t_sched, advances, in_weight, time_weight, mid_weight, out_weight):
    n = lax.axis_size("steps")
    _, lat, rows = states.shape
    ch = mid_weight.shape[0]
    pix = rows // n
    direct = pix % LANES == 0
    width = round_up(pix, LANES)
    depth = round_up(XROWS + 3 * ROUNDS * n, LANES)
    fused = (
        n <= 16 and width == TILE and ch == TILE + LANES // 2 and depth == LANES
        and (n - ITERS + 1) // 2 > LAG_NOISE and VECTOR_ROWS < ch)
    vector_rows = VECTOR_ROWS if fused else 0
    if direct:
        sent = states
        out_shape = states.shape
    else:
        sent = jnp.pad(states.reshape(lat, n, pix).transpose(1, 0, 2), ((0, 0), (0, 0), (0, width - pix)))
        out_shape = sent.shape
    vmem = pl.BlockSpec(memory_space=pltpu.VMEM)
    hbm = pl.BlockSpec(memory_space=pltpu.HBM)
    f32, bf16 = jnp.float32, jnp.bfloat16
    final, errors = pl.pallas_call(
        functools.partial(kernel, n, pix, width, depth, direct, vector_rows, fused),
        out_shape=(pltpu.VMEM(out_shape, f32), pltpu.VMEM((ROUNDS, 1, ITERS), f32)),
        in_specs=[hbm] * 9,
        out_specs=(vmem, vmem),
        scratch_shapes=[
            pltpu.SMEM(t_sched.shape, jnp.int32),
            pltpu.SMEM(advances.shape, jnp.int32),
            pltpu.SMEM((TSTEPS,), f32),
            pltpu.VMEM(sent.shape, f32),
            pltpu.VMEM((lat, ch), bf16),
            pltpu.VMEM((lat, ch), bf16),
            pltpu.VMEM((ch, ch), f32),
            pltpu.VMEM((ch, ch), bf16),
            pltpu.VMEM((2 * ch, BASE), f32),
            pltpu.VMEM((n, lat, width), f32),
            pltpu.VMEM((ITERS + 1, n, 8, width), f32),
            pltpu.VMEM((n, lat, width), f32),
            pltpu.VMEM((n, ROUNDS * ITERS, LANES), f32),
            pltpu.VMEM((n, 1, LANES), f32),
            pltpu.VMEM((n, 1, LANES), f32),
            pltpu.VMEM((16 + ch - vector_rows, LANES + depth) if fused else (ch, depth), bf16),
            pltpu.VMEM((2, ch + 16, TILE) if fused else (ch, ch), bf16),
            pltpu.VMEM((16, ch), bf16),
            pltpu.VMEM((8, ch), f32),
            pltpu.VMEM((8, ch), f32),
            pltpu.VMEM((ROUNDS * n, 8, LANES), f32),
            pltpu.VMEM((ROUNDS * n, 8, LANES), f32),
            pltpu.VMEM((lat, max(vector_rows, 8), LANES), f32),
            pltpu.VMEM((ROUNDS * n, max(vector_rows, 8), LANES), f32),
            pltpu.VMEM((lat, 8, LANES), f32),
            pltpu.VMEM((ROUNDS * n, 8, LANES), f32),
            pltpu.SemaphoreType.DMA((9,)),
        ] + [pltpu.SemaphoreType.DMA((n,))] * 6,
        compiler_params=pltpu.CompilerParams(
            collective_id=0, has_side_effects=True, vmem_limit_bytes=VMEM_BYTES),
        name="picard",
    )(*[pltpu.with_memory_space_constraint(held, pltpu.HBM) for held in (
        sent, t_sched, advances, jnp.asarray(alpha_table()), in_weight.T, out_weight, time_weight, mid_weight,
        jnp.asarray(trig_tables(time_weight.shape[1])))])
    final, errors = pl.pallas_call(
        closing,
        out_shape=(pltpu.HBM(out_shape, f32), pltpu.HBM((ROUNDS, 1, ITERS), f32)),
        in_specs=[vmem, vmem],
        out_specs=(hbm, hbm),
        scratch_shapes=[pltpu.SemaphoreType.DMA((2,))],
        compiler_params=pltpu.CompilerParams(vmem_limit_bytes=1 << 20),
        name="closing",
    )(pltpu.with_memory_space_constraint(final, pltpu.VMEM), pltpu.with_memory_space_constraint(errors, pltpu.VMEM))
    errors = errors.transpose(0, 2, 1)
    if not direct:
        final = final[:, :, :pix].transpose(1, 0, 2).reshape(states.shape)
    return final, errors


def solution(mesh):
    in_specs = (P(("groups", "steps"), None, None), P("groups"), P("groups"), P(), P(), P(), P())
    out_specs = (P(("groups", "steps"), None, None), P("groups", None, "steps"))
    return jax.shard_map(shards, mesh=mesh, in_specs=in_specs, out_specs=out_specs, check_vma=False)
```

```python
import functools
import math

import jax
import jax.numpy as jnp
import numpy as np
from jax import lax
from jax.experimental import pallas as pl
from jax.experimental.pallas import tpu as pltpu
from jax.sharding import PartitionSpec as P

TSTEPS = 1000
ITERS = 4
ROUNDS = 2
LANES = 128
BASE = 32
XROWS = 16
TILE = 256
LAG_MIXED = 1
LAG_NOISE = 3
VMEM_BYTES = 40 << 20
VECTOR_ROWS = 176


def alpha_table():
    levels = np.arange(TSTEPS, dtype=np.float64)
    low = math.sqrt(0.00085)
    high = math.sqrt(0.012)
    betas = (low + (high - low) * levels / (TSTEPS - 1)) ** 2
    return np.exp(np.cumsum(np.log1p(-betas))).astype(np.float32)


def trig_tables(width):
    half = width // 2
    freqs = np.exp(-math.log(10000.0) * np.arange(half, dtype=np.float64) / half)[:, None]
    digits = np.arange(BASE, dtype=np.float64)[None]
    high, low = freqs * digits * BASE, freqs * digits
    coarse = np.concatenate([np.cos(high), np.sin(high)]).astype(np.float32)
    fine = np.concatenate([np.cos(low), np.sin(low)]).astype(np.float32)
    return np.concatenate([coarse, fine])


def round_up(value, unit):
    return -(-value // unit) * unit


def kernel(
    n, pix, width, depth, direct, vector_rows, fused,
    states_hbm, sched_hbm, adv_hbm, alpha_hbm, inw_hbm, outw_hbm, timew_hbm, midw_hbm, trig_hbm,
    out_ref, err_ref,
    sched_ref, adv_ref, alpha_ref, states_ref, inw_ref, outw_ref, timew, midw, trig, xin, xs, fin, final_in, errs, lhs, mid, outs, outw, inw, coef_one, coef_two,
    in_table, time_table, linear_in, linear_time, hot_table,
    local, in_send, in_recv, out_send, out_recv,
):
    lat = outw_ref.shape[0]
    ch = midw.shape[0]
    me = lax.axis_index("steps")
    span = ROUNDS * n
    f32, bf16 = jnp.float32, jnp.bfloat16

    def peer(hop):
        if n > 16 or n & (n - 1):
            return lax.rem(me + hop, n)
        other = me
        for bit in range(n.bit_length() - 1):
            if hop >> bit & 1:
                digit = lax.rem(lax.div(me, 1 << bit), 2)
                other = other + (1 << bit) * (1 - 2 * digit)
        return other

    def source(d):
        if direct:
            return states_ref.at[0, :, pl.ds(pl.multiple_of(d * pix, LANES), pix)]
        return states_ref.at[d]

    def in_copy(d, slot):
        return pltpu.make_async_remote_copy(
            src_ref=source(d), dst_ref=xin.at[slot], send_sem=in_send.at[d], recv_sem=in_recv.at[slot],
            device_id={"steps": d}, device_id_type=pl.DeviceIdType.MESH)

    def out_copy(d, slot):
        return pltpu.make_async_remote_copy(
            src_ref=fin.at[d], dst_ref=final_in.at[slot], send_sem=out_send.at[d], recv_sem=out_recv.at[slot],
            device_id={"steps": d}, device_id_type=pl.DeviceIdType.MESH)

    def each_peer(act):
        if n <= 16:
            for hop in reversed(range(1, n)):
                act(peer(hop))
        else:
            @pl.loop(1, n)
            def _(hop):
                act(peer(hop))

    loads = [
        pltpu.make_async_copy(source_ref, held, local.at[j])
        for j, (source_ref, held) in enumerate((
            (states_hbm, states_ref), (sched_hbm, sched_ref), (adv_hbm, adv_ref), (alpha_hbm, alpha_ref),
            (trig_hbm, trig), (timew_hbm, timew), (midw_hbm, midw), (inw_hbm, inw_ref), (outw_hbm, outw_ref)))
    ]
    loads[0].start()
    barrier = pltpu.get_barrier_semaphore()
    each_peer(lambda d: pl.semaphore_signal(
        barrier, inc=1, device_id={"steps": d}, device_id_type=pl.DeviceIdType.MESH))
    for load in loads[1:]:
        load.start()
    loads[0].wait()
    pl.semaphore_wait(barrier, n - 1)
    each_peer(lambda d: in_copy(d, me).start())

    for load in loads[1:4]:
        load.wait()
    lane = lax.broadcasted_iota(jnp.int32, (1, depth), 1) - XROWS
    member = jnp.where((lane >= 0) & (lane < 3 * span), lax.rem(jnp.maximum(lane, 0), span), -1)
    advance_one = adv_ref[0]

    def coefficients(m, stamps):
        place = jnp.where(m >= n, advance_one + m - n, m)
        now, after = sched_ref[place], sched_ref[place + 1]
        a_now = jnp.full((8, LANES), alpha_ref[now], f32)
        a_after = jnp.full((8, LANES), alpha_ref[after], f32)
        one = jnp.sqrt(a_after / a_now)
        two = jnp.sqrt(1.0 - a_after) - one * jnp.sqrt(1.0 - a_now)
        coef_one[m] = one - 1.0
        coef_two[m] = two
        return jnp.where(member == m, now, stamps)

    stamps = lax.fori_loop(0, span, coefficients, jnp.zeros((1, depth), jnp.int32), unroll=8)

    digit = lax.broadcasted_iota(jnp.int32, (BASE, depth), 0)
    hot_high = (digit == lax.shift_right_logical(stamps, 5)).astype(f32)
    hot_low = (digit == lax.bitwise_and(stamps, BASE - 1)).astype(f32)
    exact = lax.Precision.HIGHEST
    for load in loads[4:]:
        load.wait()
    high = jnp.dot(trig[0:ch], hot_high, precision=exact, preferred_element_type=f32)
    low = jnp.dot(trig[ch:], hot_low, precision=exact, preferred_element_type=f32)
    half = ch // 2
    cos_h, sin_h, cos_l, sin_l = high[:half], high[half:], low[:half], low[half:]
    feats = jnp.concatenate([cos_h * cos_l - sin_h * sin_l, sin_h * cos_l + cos_h * sin_l], axis=0)
    embed = jnp.dot(timew[...], feats, precision=exact, preferred_element_type=f32)
    inw[...] = jnp.zeros_like(inw)
    inw[0:lat, :] = inw_ref[...].astype(f32)
    unit = (lax.broadcasted_iota(jnp.int32, (8, depth), 0) == lane + XROWS).astype(f32)
    spread = lax.dot_general(
        inw[...], unit, (((0,), (0,)), ((), ())), precision=exact, preferred_element_type=f32)
    top = embed.astype(bf16).astype(f32)
    rest = embed - top
    middle = rest.astype(bf16).astype(f32)
    bottom = (rest - middle).astype(bf16).astype(f32)
    part = jnp.where(lane < span, top, jnp.where(lane < 2 * span, middle, bottom))
    part = jnp.where(member >= 0, part, 0.0)
    left = spread + part
    matrix_rows = ch - vector_rows
    outw[...] = jnp.zeros_like(outw)
    outw[0:lat, :] = outw_ref[...].astype(f32)
    half_mid = (midw[...].astype(f32) * 0.5).astype(bf16)
    whole = spread + jnp.where(member >= 0, embed, 0.0)
    linear = jnp.dot(outw[...], whole, precision=exact, preferred_element_type=f32)

    def folded(high, low):
        return jnp.concatenate([jnp.zeros_like(high), high + pltpu.roll(low, lat, axis=0)], axis=0).astype(bf16)

    padded_out = jnp.concatenate([outw[...], jnp.zeros_like(outw[...])], axis=0).astype(bf16)
    narrow = lambda rows, lanes: jnp.zeros((rows, lanes), bf16)
    cuts_one = (0, TILE - LANES // 2, ch)
    cuts_two = (0, LANES // 2, TILE - (ch - cuts_one[1]) + LANES // 2, ch)
    if fused:
        both_out = jnp.dot(padded_out, half_mid, preferred_element_type=f32)[0:8]
        both_top = both_out.astype(bf16).astype(f32)
        passed = folded(both_top, both_out - both_top)
        for part in range(2):
            one = half_mid[:, cuts_one[part]:cuts_one[part + 1]]
            two = padded_out[:, cuts_two[part]:cuts_two[part + 1]]
            mid[part, 0:ch, :] = jnp.concatenate([one, narrow(ch, two.shape[1])], axis=1)
            through = passed[:, cuts_one[part]:cuts_one[part + 1]]
            mid[part, ch:, :] = jnp.concatenate([through, two], axis=1)
        lhs[0:16, 0:LANES] = padded_out[:, cuts_two[2]:]
        line_top = linear.astype(bf16).astype(f32)
        line_rest = linear - line_top
        line_middle = line_rest.astype(bf16).astype(f32)
        line_bottom = line_rest - line_middle
        line = jnp.where(lane < span, line_top, jnp.where(lane < 2 * span, line_middle, line_bottom))
        lhs[0:16, LANES:] = folded(
            jnp.where((member >= 0) | (lane < 0), line, 0.0), jnp.where(lane < 0, line_middle, 0.0))
        lhs[16:, 0:LANES] = narrow(matrix_rows, LANES)
        lhs[16:, LANES:] = left[0:matrix_rows].astype(bf16)
    else:
        mid[...] = half_mid
        outs[...] = padded_out
        lhs[...] = left[0:matrix_rows].astype(bf16)
    for l in range(lat):
        if not fused:
            linear_in[l] = jnp.broadcast_to(linear[:, l:l + 1], (8, LANES))
        if vector_rows:
            in_table[l] = jnp.broadcast_to(whole[matrix_rows:, l:l + 1], (vector_rows, LANES))
    for m in range(span):
        at = XROWS + m
        if not fused:
            linear_time[m] = jnp.broadcast_to(linear[:, at:at + 1], (8, LANES))
        if vector_rows:
            time_table[m] = jnp.broadcast_to(whole[matrix_rows:, at:at + 1], (vector_rows, LANES))

    hot_row = lax.broadcasted_iota(jnp.int32, (depth - XROWS, LANES), 0)
    hot_member = jnp.where(hot_row < 3 * span, lax.rem(hot_row, span), -1)
    if fused:
        for m in range(span):
            hot_table[m] = (hot_member == m).astype(f32).astype(bf16)
    copies = 2 if fused else 1
    if not fused:
        xs[0] = jnp.zeros_like(xs[0])
    errs[...] = jnp.zeros_like(errs)

    def place(d, values):
        for copy in range(copies):
            xs[0, d, copy * lat:(copy + 1) * lat, :] = values

    place(me, states_ref[0, :, pl.ds(pl.multiple_of(me * pix, LANES), pix)] if direct else states_ref[me])

    def arrived(d):
        in_copy(d, d).wait_recv()
        place(d, xin[d])

    each_peer(arrived)

    wide = lambda tile: jnp.concatenate([tile] * (width // LANES), axis=1) if width > LANES else tile

    def swish(full):
        return full * jax.nn.sigmoid(full)

    def bent(half):
        return half * jnp.tanh(half)

    join = lambda parts: parts[0] if len(parts) == 1 else jnp.concatenate(parts, axis=1)
    tiles = [slice(start, start + LANES) for start in range(0, width, LANES)]

    def affine(base, slopes, x, tile):
        total = base
        for l in range(lat):
            total = total + slopes[l] * x[l:l + 1, tile]
        return total

    def column(x, m):
        hot = wide(hot_table[m] if fused else (hot_member == m).astype(f32).astype(bf16))
        padded = jnp.concatenate([x, jnp.zeros((XROWS - 8, width), f32)], axis=0).astype(bf16)
        return jnp.concatenate([padded, hot], axis=0)

    def vector_part(x, m):
        rounded = x.astype(bf16).astype(f32)
        return join([swish(affine(time_table[m], in_table, rounded, tile).astype(bf16)) for tile in tiles])

    def linear_part(x, m):
        rounded = x.astype(bf16).astype(f32)
        return join([affine(linear_time[m], linear_in, rounded, tile) for tile in tiles])

    def product(weights, values):
        return jnp.dot(weights, values, preferred_element_type=f32)

    def note_error(row, k, change):
        square = change * change
        if pix < width:
            square = jnp.where(lax.broadcasted_iota(jnp.int32, square.shape, 1) < pix, square, 0.0)
        total = square[:, 0:LANES]
        for start in range(LANES, width, LANES):
            total = total + square[:, start:start + LANES]
        errs[k, pl.ds(row, 1), :] = jnp.sum(total, axis=0, keepdims=True)

    def moved(r, m_at, old, noise):
        return wide(coef_one[m_at]) * old + wide(coef_two[m_at]) * noise

    def flat_round(r):
        todo = [(i, k) for i in range(ITERS) for k in range(i, n - 1)]
        groups = [todo[j:j + 2] for j in range(0, len(todo), 2)]
        count = len(groups)
        tails, hidden, late, running, straight = {}, {}, {}, {}, {}

        def finish(i, k, noise):
            row = r * ITERS + i
            old = xs[i, k]
            if k == i:
                running[i] = old
                xs[ITERS, k] = old
            running[i] = running[i] + moved(r, r * n + k, old, noise)
            note_error(row, k + 1, running[i] - xs[i, k + 1])
            xs[i + 1, k + 1] = running[i]

        def pad(values, lanes):
            return values if values.shape[1] == lanes else jnp.concatenate(
                [values, jnp.zeros((values.shape[0], lanes - values.shape[1]), bf16)], axis=1)

        for step in range(count + LAG_NOISE):
            new, second, third = step, step - LAG_MIXED, step - LAG_NOISE
            has_new, has_second, has_third = new < count, 0 <= second < count, 0 <= third < count
            sizes = [len(groups[g]) * width for g, there in ((new, has_new), (second, has_second), (third, has_third)) if there]
            lanes = max(sizes)
            noise = mixed = None
            if has_new:
                now, extras = [], []
                for i, k in groups[new]:
                    x = xs[i, k]
                    now.append(column(x, r * n + k))
                    extras.append(vector_part(x, r * n + k))
                new_rows = pad(join(now), lanes)
            else:
                new_rows = jnp.zeros((depth, lanes), bf16)
            old_rows = pad(late[third], lanes) if has_third else jnp.zeros((ch, lanes), bf16)
            mid_rows = pad(hidden[second], lanes) if has_second else jnp.zeros((ch, lanes), bf16)
            if has_new or has_third:
                end = lhs.shape[0] if has_new else 16
                both = product(lhs[0:end], jnp.concatenate([old_rows[cuts_two[2]:], new_rows], axis=0))
                if has_new:
                    tails[new] = both[8:16]
                    hid = swish(both[16:, 0:len(groups[new]) * width].astype(bf16))
                    hidden[new] = jnp.concatenate([hid, join(extras)], axis=0) if vector_rows else hid
                if has_third:
                    noise = both[0:8]
            if has_second or has_third:
                begin = 0 if has_second else ch
                for part in range(2):
                    values = jnp.concatenate([
                        mid_rows[cuts_one[part]:cuts_one[part + 1]], old_rows[cuts_two[part]:cuts_two[part + 1]]], axis=0)
                    both = product(mid[part, begin:], values)
                    if has_second:
                        mixed = both[0:ch] if mixed is None else mixed + both[0:ch]
                        line = both[ch + 8:ch + 16]
                        straight[second] = straight[second] + line if second in straight else line
                    if has_third:
                        noise = noise + both[ch - begin:ch - begin + 8]
            if has_second:
                late[second] = bent(mixed[:, 0:len(groups[second]) * width].astype(bf16))
                del hidden[second]
            if has_third:
                for j, (i, k) in enumerate(groups[third]):
                    at = slice(j * width, (j + 1) * width)
                    total = tails[third][:, at] + straight[third][:, at] + noise[:, at]
                    finish(i, k, total + pltpu.roll(total, lat, axis=0))
                del late[third]

    def rolled_round(r):
        for i in range(ITERS):
            row = r * ITERS + i

            def body(k, running):
                old = xs[0, k]
                tail = linear_part(old, r * n + k)
                hid = swish(product(lhs[...], column(old, r * n + k)).astype(bf16))
                half = product(mid[...], hid).astype(bf16)
                noise = tail + product(outs[...], half + bent(half))[0:8]
                note_error(row, k, running - old)
                xs[0, k] = running
                return running + moved(r, r * n + k, old, noise)

            running = lax.fori_loop(i, n - 1, body, xs[0, i])
            note_error(row, n - 1, running - xs[0, n - 1])
            xs[0, n - 1] = running

    def one_round(r, carry):
        advance = adv_ref[r]
        if fused:
            flat_round(r)
            for k in range(n):
                xs[0, k] = xs[ITERS, jnp.minimum(k + advance, n - 1)]
        else:
            rolled_round(r)

            def shift(k, carry):
                xs[0, k] = xs[0, jnp.minimum(k + advance, n - 1)]
                return carry

            lax.fori_loop(0, n, shift, 0, unroll=4)
        return carry

    lax.fori_loop(0, ROUNDS, one_round, 0)
    cells = (ROUNDS * ITERS, LANES)
    diagonal = lax.broadcasted_iota(jnp.int32, cells, 0) == lax.broadcasted_iota(jnp.int32, cells, 1)
    fin[...] = jnp.zeros_like(fin)
    for k in range(n):
        total = jnp.sum(errs[k], axis=1, keepdims=True)
        fin[k, :, 0:width] = xs[0, k, 0:lat, :]
        fin[k, 0:1, width:] = jnp.sum(jnp.where(diagonal, total, 0.0), axis=0, keepdims=True)
    each_peer(lambda d: out_copy(d, me).start())
    final_in[me] = fin[me]
    each_peer(lambda d: out_copy(d, d).wait_recv())
    sums = jnp.zeros((1, LANES), f32)
    for d in range(n):
        sums = sums + final_in[d, 0:1, width:]
        if direct:
            out_ref[0, :, d * pix:(d + 1) * pix] = final_in[d, :, 0:pix]
        else:
            out_ref[d] = final_in[d, :, 0:width]
    means = sums * (1.0 / (copies * lat * n * pix))
    for r in range(ROUNDS):
        err_ref[r] = means[:, r * ITERS:(r + 1) * ITERS]
    each_peer(lambda d: in_copy(d, me).wait_send())
    each_peer(lambda d: out_copy(d, me).wait_send())


def closing(final_ref, errors_ref, final_out, errors_out, sems):
    copies = [
        pltpu.make_async_copy(final_ref, final_out, sems.at[0]),
        pltpu.make_async_copy(errors_ref, errors_out, sems.at[1]),
    ]
    for copy in copies:
        copy.start()
    for copy in copies:
        copy.wait()


def shards(states, t_sched, advances, in_weight, time_weight, mid_weight, out_weight):
    n = lax.axis_size("steps")
    _, lat, rows = states.shape
    ch = mid_weight.shape[0]
    pix = rows // n
    direct = pix % LANES == 0
    width = round_up(pix, LANES)
    depth = round_up(XROWS + 3 * ROUNDS * n, LANES)
    fused = (
        n <= 16 and width == TILE and ch == TILE + LANES // 2 and depth == LANES
        and (n - ITERS + 1) // 2 > LAG_NOISE and 0 < VECTOR_ROWS < ch and 2 * lat == 8)
    vector_rows = VECTOR_ROWS if fused else 0
    if direct:
        sent = states
        out_shape = states.shape
    else:
        sent = jnp.pad(states.reshape(lat, n, pix).transpose(1, 0, 2), ((0, 0), (0, 0), (0, width - pix)))
        out_shape = sent.shape
    vmem = pl.BlockSpec(memory_space=pltpu.VMEM)
    hbm = pl.BlockSpec(memory_space=pltpu.HBM)
    f32, bf16 = jnp.float32, jnp.bfloat16
    final, errors = pl.pallas_call(
        functools.partial(kernel, n, pix, width, depth, direct, vector_rows, fused),
        out_shape=(pltpu.VMEM(out_shape, f32), pltpu.VMEM((ROUNDS, 1, ITERS), f32)),
        in_specs=[hbm] * 9,
        out_specs=(vmem, vmem),
        scratch_shapes=[
            pltpu.SMEM(t_sched.shape, jnp.int32),
            pltpu.SMEM(advances.shape, jnp.int32),
            pltpu.SMEM((TSTEPS,), f32),
            pltpu.VMEM(sent.shape, f32),
            pltpu.VMEM((lat, ch), bf16),
            pltpu.VMEM((lat, ch), bf16),
            pltpu.VMEM((ch, ch), f32),
            pltpu.VMEM((ch, ch), bf16),
            pltpu.VMEM((2 * ch, BASE), f32),
            pltpu.VMEM((n, lat, width), f32),
            pltpu.VMEM((ITERS + 1, n, 8, width), f32),
            pltpu.VMEM((n, lat, width + LANES), f32),
            pltpu.VMEM((n, lat, width + LANES), f32),
            pltpu.VMEM((n, ROUNDS * ITERS, LANES), f32),
            pltpu.VMEM((16 + ch - vector_rows, LANES + depth) if fused else (ch, depth), bf16),
            pltpu.VMEM((2, ch + 16, TILE) if fused else (ch, ch), bf16),
            pltpu.VMEM((16, ch), bf16),
            pltpu.VMEM((8, ch), f32),
            pltpu.VMEM((8, ch), f32),
            pltpu.VMEM((ROUNDS * n, 8, LANES), f32),
            pltpu.VMEM((ROUNDS * n, 8, LANES), f32),
            pltpu.VMEM((lat, max(vector_rows, 8), LANES), f32),
            pltpu.VMEM((ROUNDS * n, max(vector_rows, 8), LANES), f32),
            pltpu.VMEM((lat, 8, LANES), f32),
            pltpu.VMEM((ROUNDS * n, 8, LANES), f32),
            pltpu.VMEM((ROUNDS * n if fused else 1, depth - XROWS, LANES), bf16),
            pltpu.SemaphoreType.DMA((9,)),
        ] + [pltpu.SemaphoreType.DMA((n,))] * 4,
        compiler_params=pltpu.CompilerParams(
            collective_id=0, has_side_effects=True, vmem_limit_bytes=VMEM_BYTES),
        name="picard",
    )(*[pltpu.with_memory_space_constraint(held, pltpu.HBM) for held in (
        sent, t_sched, advances, jnp.asarray(alpha_table()), in_weight.T, out_weight, time_weight, mid_weight,
        jnp.asarray(trig_tables(time_weight.shape[1])))])
    final, errors = pl.pallas_call(
        closing,
        out_shape=(pltpu.HBM(out_shape, f32), pltpu.HBM((ROUNDS, 1, ITERS), f32)),
        in_specs=[vmem, vmem],
        out_specs=(hbm, hbm),
        scratch_shapes=[pltpu.SemaphoreType.DMA((2,))],
        compiler_params=pltpu.CompilerParams(vmem_limit_bytes=1 << 20),
        name="closing",
    )(pltpu.with_memory_space_constraint(final, pltpu.VMEM), pltpu.with_memory_space_constraint(errors, pltpu.VMEM))
    errors = errors.transpose(0, 2, 1)
    if not direct:
        final = final[:, :, :pix].transpose(1, 0, 2).reshape(states.shape)
    return final, errors


def solution(mesh):
    in_specs = (P(("groups", "steps"), None, None), P("groups"), P("groups"), P(), P(), P(), P())
    out_specs = (P(("groups", "steps"), None, None), P("groups", None, "steps"))
    return jax.shard_map(shards, mesh=mesh, in_specs=in_specs, out_specs=out_specs, check_vma=False)
```

```python
import functools
import math

import jax
import jax.numpy as jnp
import numpy as np
from jax import lax
from jax.experimental import pallas as pl
from jax.experimental.pallas import tpu as pltpu
from jax.sharding import PartitionSpec as P

TSTEPS = 1000
ITERS = 4
ROUNDS = 2
LANES = 128
BASE = 32
XROWS = 16
TILE = 256
LAG_MIXED = 1
LAG_NOISE = 3
VMEM_BYTES = 40 << 20
VECTOR_ROWS = 176


def alpha_table():
    levels = np.arange(TSTEPS, dtype=np.float64)
    low = math.sqrt(0.00085)
    high = math.sqrt(0.012)
    betas = (low + (high - low) * levels / (TSTEPS - 1)) ** 2
    return np.exp(np.cumsum(np.log1p(-betas))).astype(np.float32)


def trig_tables(width):
    half = width // 2
    freqs = np.exp(-math.log(10000.0) * np.arange(half, dtype=np.float64) / half)[:, None]
    digits = np.arange(BASE, dtype=np.float64)[None]
    high, low = freqs * digits * BASE, freqs * digits
    coarse = np.concatenate([np.cos(high), np.sin(high)]).astype(np.float32)
    fine = np.concatenate([np.cos(low), np.sin(low)]).astype(np.float32)
    return np.concatenate([coarse, fine])


def round_up(value, unit):
    return -(-value // unit) * unit


def kernel(
    n, pix, width, depth, direct, vector_rows, fused,
    states_hbm, sched_hbm, adv_hbm, alpha_hbm, inw_hbm, outw_hbm, timew_hbm, midw_hbm, trig_hbm,
    out_ref, err_ref,
    sched_ref, adv_ref, alpha_ref, states_ref, inw_ref, outw_ref, timew, midw, trig, xin, xs, fin, final_in, errs, lhs, mid, outs, outw, inw, coef_one, coef_two,
    in_table, time_table, linear_in, linear_time, hot_table,
    local, in_send, in_recv, out_send, out_recv,
):
    lat = outw_ref.shape[0]
    ch = midw.shape[0]
    me = lax.axis_index("steps")
    span = ROUNDS * n
    f32, bf16 = jnp.float32, jnp.bfloat16

    def peer(hop):
        if n > 16 or n & (n - 1):
            return lax.rem(me + hop, n)
        other = me
        for bit in range(n.bit_length() - 1):
            if hop >> bit & 1:
                digit = lax.rem(lax.div(me, 1 << bit), 2)
                other = other + (1 << bit) * (1 - 2 * digit)
        return other

    def source(d):
        if direct:
            return states_ref.at[0, :, pl.ds(pl.multiple_of(d * pix, LANES), pix)]
        return states_ref.at[d]

    def in_copy(d, slot):
        return pltpu.make_async_remote_copy(
            src_ref=source(d), dst_ref=xin.at[slot], send_sem=in_send.at[d], recv_sem=in_recv.at[slot],
            device_id={"steps": d}, device_id_type=pl.DeviceIdType.MESH)

    def out_copy(d, slot):
        return pltpu.make_async_remote_copy(
            src_ref=fin.at[d], dst_ref=final_in.at[slot], send_sem=out_send.at[d], recv_sem=out_recv.at[slot],
            device_id={"steps": d}, device_id_type=pl.DeviceIdType.MESH)

    def each_peer(act, near_first=False):
        if n <= 16:
            for hop in range(1, n) if near_first else reversed(range(1, n)):
                act(peer(hop))
        else:
            @pl.loop(1, n)
            def _(hop):
                act(peer(hop))

    loads = [
        pltpu.make_async_copy(source_ref, held, local.at[j])
        for j, (source_ref, held) in enumerate((
            (states_hbm, states_ref), (sched_hbm, sched_ref), (adv_hbm, adv_ref), (alpha_hbm, alpha_ref),
            (trig_hbm, trig), (timew_hbm, timew), (midw_hbm, midw), (inw_hbm, inw_ref), (outw_hbm, outw_ref)))
    ]
    loads[0].start()
    barrier = pltpu.get_barrier_semaphore()
    each_peer(lambda d: pl.semaphore_signal(
        barrier, inc=1, device_id={"steps": d}, device_id_type=pl.DeviceIdType.MESH))
    for load in loads[1:]:
        load.start()
    loads[0].wait()
    pl.semaphore_wait(barrier, n - 1)
    each_peer(lambda d: in_copy(d, me).start())

    for load in loads[1:4]:
        load.wait()
    lane = lax.broadcasted_iota(jnp.int32, (1, depth), 1) - XROWS
    member = jnp.where((lane >= 0) & (lane < 3 * span), lax.rem(jnp.maximum(lane, 0), span), -1)
    advance_one = adv_ref[0]

    def coefficients(m, stamps):
        place = jnp.where(m >= n, advance_one + m - n, m)
        now, after = sched_ref[place], sched_ref[place + 1]
        a_now = jnp.full((8, LANES), alpha_ref[now], f32)
        a_after = jnp.full((8, LANES), alpha_ref[after], f32)
        one = jnp.sqrt(a_after / a_now)
        two = jnp.sqrt(1.0 - a_after) - one * jnp.sqrt(1.0 - a_now)
        coef_one[m] = one - 1.0
        coef_two[m] = two
        return jnp.where(member == m, now, stamps)

    stamps = lax.fori_loop(0, span, coefficients, jnp.zeros((1, depth), jnp.int32), unroll=8)

    digit = lax.broadcasted_iota(jnp.int32, (BASE, depth), 0)
    hot_high = (digit == lax.shift_right_logical(stamps, 5)).astype(f32)
    hot_low = (digit == lax.bitwise_and(stamps, BASE - 1)).astype(f32)
    exact = lax.Precision.HIGHEST
    for load in loads[4:]:
        load.wait()
    high = jnp.dot(trig[0:ch], hot_high, precision=exact, preferred_element_type=f32)
    low = jnp.dot(trig[ch:], hot_low, precision=exact, preferred_element_type=f32)
    half = ch // 2
    cos_h, sin_h, cos_l, sin_l = high[:half], high[half:], low[:half], low[half:]
    feats = jnp.concatenate([cos_h * cos_l - sin_h * sin_l, sin_h * cos_l + cos_h * sin_l], axis=0)
    embed = jnp.dot(timew[...], feats, precision=exact, preferred_element_type=f32)
    inw[...] = jnp.zeros_like(inw)
    inw[0:lat, :] = inw_ref[...].astype(f32)
    unit = (lax.broadcasted_iota(jnp.int32, (8, depth), 0) == lane + XROWS).astype(f32)
    spread = lax.dot_general(
        inw[...], unit, (((0,), (0,)), ((), ())), precision=exact, preferred_element_type=f32)
    top = embed.astype(bf16).astype(f32)
    rest = embed - top
    middle = rest.astype(bf16).astype(f32)
    bottom = (rest - middle).astype(bf16).astype(f32)
    part = jnp.where(lane < span, top, jnp.where(lane < 2 * span, middle, bottom))
    part = jnp.where(member >= 0, part, 0.0)
    left = spread + part
    matrix_rows = ch - vector_rows
    outw[...] = jnp.zeros_like(outw)
    outw[0:lat, :] = outw_ref[...].astype(f32)
    half_mid = (midw[...].astype(f32) * 0.5).astype(bf16)
    whole = spread + jnp.where(member >= 0, embed, 0.0)
    linear = jnp.dot(outw[...], whole, precision=exact, preferred_element_type=f32)

    def folded(high, low):
        return jnp.concatenate([jnp.zeros_like(high), high + pltpu.roll(low, lat, axis=0)], axis=0).astype(bf16)

    padded_out = jnp.concatenate([outw[...], jnp.zeros_like(outw[...])], axis=0).astype(bf16)
    narrow = lambda rows, lanes: jnp.zeros((rows, lanes), bf16)
    cuts_one = (0, TILE - LANES // 2, ch)
    cuts_two = (0, LANES // 2, TILE - (ch - cuts_one[1]) + LANES // 2, ch)
    if fused:
        both_out = jnp.dot(padded_out, half_mid, preferred_element_type=f32)[0:8]
        both_top = both_out.astype(bf16).astype(f32)
        passed = folded(both_top, both_out - both_top)
        for part in range(2):
            one = half_mid[:, cuts_one[part]:cuts_one[part + 1]]
            two = padded_out[:, cuts_two[part]:cuts_two[part + 1]]
            mid[part, 0:ch, :] = jnp.concatenate([one, narrow(ch, two.shape[1])], axis=1)
            through = passed[:, cuts_one[part]:cuts_one[part + 1]]
            mid[part, ch:, :] = jnp.concatenate([through, two], axis=1)
        lhs[0:16, 0:LANES] = padded_out[:, cuts_two[2]:]
        line_top = linear.astype(bf16).astype(f32)
        line_rest = linear - line_top
        line_middle = line_rest.astype(bf16).astype(f32)
        line_bottom = line_rest - line_middle
        line = jnp.where(lane < span, line_top, jnp.where(lane < 2 * span, line_middle, line_bottom))
        lhs[0:16, LANES:] = folded(
            jnp.where((member >= 0) | (lane < 0), line, 0.0), jnp.where(lane < 0, line_middle, 0.0))
        lhs[16:, 0:LANES] = narrow(matrix_rows, LANES)
        lhs[16:, LANES:] = left[0:matrix_rows].astype(bf16)
    else:
        mid[...] = half_mid
        outs[...] = padded_out
        lhs[...] = left[0:matrix_rows].astype(bf16)
    for l in range(lat):
        if not fused:
            linear_in[l] = jnp.broadcast_to(linear[:, l:l + 1], (8, LANES))
        if vector_rows:
            in_table[l] = jnp.broadcast_to(whole[matrix_rows:, l:l + 1], (vector_rows, LANES))
    for m in range(span):
        at = XROWS + m
        if not fused:
            linear_time[m] = jnp.broadcast_to(linear[:, at:at + 1], (8, LANES))
        if vector_rows:
            time_table[m] = jnp.broadcast_to(whole[matrix_rows:, at:at + 1], (vector_rows, LANES))

    hot_row = lax.broadcasted_iota(jnp.int32, (depth - XROWS, LANES), 0)
    hot_member = jnp.where(hot_row < 3 * span, lax.rem(hot_row, span), -1)
    if fused:
        for m in range(span):
            hot_table[m] = (hot_member == m).astype(f32).astype(bf16)
    copies = 2 if fused else 1
    if not fused:
        xs[0] = jnp.zeros_like(xs[0])
    errs[...] = jnp.zeros_like(errs)

    def place(d, values):
        for copy in range(copies):
            xs[ITERS if fused else 0, d, copy * lat:(copy + 1) * lat, :] = values

    place(me, states_ref[0, :, pl.ds(pl.multiple_of(me * pix, LANES), pix)] if direct else states_ref[me])

    def arrived(d):
        in_copy(d, d).wait_recv()
        place(d, xin[d])

    each_peer(arrived, near_first=True)

    wide = lambda tile: jnp.concatenate([tile] * (width // LANES), axis=1) if width > LANES else tile

    def swish(full):
        return full * jax.nn.sigmoid(full)

    def bent(half):
        return half * jnp.tanh(half)

    join = lambda parts: parts[0] if len(parts) == 1 else jnp.concatenate(parts, axis=1)
    tiles = [slice(start, start + LANES) for start in range(0, width, LANES)]

    def affine(base, slopes, x, tile):
        total = base
        for l in range(lat):
            total = total + slopes[l] * x[l:l + 1, tile]
        return total

    def column(x, m):
        hot = wide(hot_table[m] if fused else (hot_member == m).astype(f32).astype(bf16))
        padded = jnp.concatenate([x, jnp.zeros((XROWS - 8, width), f32)], axis=0).astype(bf16)
        return jnp.concatenate([padded, hot], axis=0)

    def vector_part(x, m):
        rounded = x.astype(bf16).astype(f32)
        return join([swish(affine(time_table[m], in_table, rounded, tile).astype(bf16)) for tile in tiles])

    def linear_part(x, m):
        rounded = x.astype(bf16).astype(f32)
        return join([affine(linear_time[m], linear_in, rounded, tile) for tile in tiles])

    def product(weights, values):
        return jnp.dot(weights, values, preferred_element_type=f32)

    def note_error(row, k, change):
        square = change * change
        if pix < width:
            square = jnp.where(lax.broadcasted_iota(jnp.int32, square.shape, 1) < pix, square, 0.0)
        total = square[:, 0:LANES]
        for start in range(LANES, width, LANES):
            total = total + square[:, start:start + LANES]
        whole_sum = jnp.sum(jnp.sum(total, axis=0, keepdims=True), axis=1, keepdims=True)
        errs[k, pl.ds(row, 1), :] = jnp.broadcast_to(whole_sum, (1, LANES))

    def moved(r, m_at, old, noise):
        return wide(coef_one[m_at]) * old + wide(coef_two[m_at]) * noise

    def flat_round(r):
        todo = [(i, k) for i in range(ITERS) for k in range(i, n - 1)]
        groups = [todo[j:j + 2] for j in range(0, len(todo), 2)]
        count = len(groups)
        tails, hidden, late, running, straight = {}, {}, {}, {}, {}

        def finish(i, k, noise):
            row = r * ITERS + i
            old = xs[i, k]
            if k == i:
                running[i] = old
                xs[ITERS, k] = old
            running[i] = running[i] + moved(r, r * n + k, old, noise)
            note_error(row, k + 1, running[i] - xs[i, k + 1])
            xs[i + 1, k + 1] = running[i]

        def pad(values, lanes):
            return values if values.shape[1] == lanes else jnp.concatenate(
                [values, jnp.zeros((values.shape[0], lanes - values.shape[1]), bf16)], axis=1)

        for step in range(count + LAG_NOISE):
            new, second, third = step, step - LAG_MIXED, step - LAG_NOISE
            has_new, has_second, has_third = new < count, 0 <= second < count, 0 <= third < count
            sizes = [len(groups[g]) * width for g, there in ((new, has_new), (second, has_second), (third, has_third)) if there]
            lanes = max(sizes)
            noise = mixed = None
            if has_new:
                now, extras = [], []
                for i, k in groups[new]:
                    x = xs[i, k]
                    now.append(column(x, r * n + k))
                    extras.append(vector_part(x, r * n + k))
                new_rows = pad(join(now), lanes)
            else:
                new_rows = jnp.zeros((depth, lanes), bf16)
            old_rows = pad(late[third], lanes) if has_third else jnp.zeros((ch, lanes), bf16)
            mid_rows = pad(hidden[second], lanes) if has_second else jnp.zeros((ch, lanes), bf16)
            if has_new or has_third:
                end = lhs.shape[0] if has_new else 16
                both = product(lhs[0:end], jnp.concatenate([old_rows[cuts_two[2]:], new_rows], axis=0))
                if has_new:
                    tails[new] = both[8:16]
                    hid = swish(both[16:, 0:len(groups[new]) * width].astype(bf16))
                    hidden[new] = jnp.concatenate([hid, join(extras)], axis=0) if vector_rows else hid
                if has_third:
                    noise = both[0:8]
            if has_second or has_third:
                begin = 0 if has_second else ch
                for part in range(2):
                    values = jnp.concatenate([
                        mid_rows[cuts_one[part]:cuts_one[part + 1]], old_rows[cuts_two[part]:cuts_two[part + 1]]], axis=0)
                    both = product(mid[part, begin:], values)
                    if has_second:
                        mixed = both[0:ch] if mixed is None else mixed + both[0:ch]
                        line = both[ch + 8:ch + 16]
                        straight[second] = straight[second] + line if second in straight else line
                    if has_third:
                        noise = noise + both[ch - begin:ch - begin + 8]
            if has_second:
                late[second] = bent(mixed[:, 0:len(groups[second]) * width].astype(bf16))
                del hidden[second]
            if has_third:
                for j, (i, k) in enumerate(groups[third]):
                    at = slice(j * width, (j + 1) * width)
                    total = tails[third][:, at] + straight[third][:, at] + noise[:, at]
                    finish(i, k, total + pltpu.roll(total, lat, axis=0))
                del late[third]

    def rolled_round(r):
        for i in range(ITERS):
            row = r * ITERS + i

            def body(k, running):
                old = xs[0, k]
                tail = linear_part(old, r * n + k)
                hid = swish(product(lhs[...], column(old, r * n + k)).astype(bf16))
                half = product(mid[...], hid).astype(bf16)
                noise = tail + product(outs[...], half + bent(half))[0:8]
                note_error(row, k, running - old)
                xs[0, k] = running
                return running + moved(r, r * n + k, old, noise)

            running = lax.fori_loop(i, n - 1, body, xs[0, i])
            note_error(row, n - 1, running - xs[0, n - 1])
            xs[0, n - 1] = running

    def one_round(r, carry):
        advance = adv_ref[r]
        if fused:
            behind = jnp.where(r == 0, 0, adv_ref[jnp.maximum(r - 1, 0)])
            for k in range(n):
                xs[0, k] = xs[ITERS, jnp.minimum(k + behind, n - 1)]
            flat_round(r)
        else:
            rolled_round(r)

            def shift(k, carry):
                xs[0, k] = xs[0, jnp.minimum(k + advance, n - 1)]
                return carry

            lax.fori_loop(0, n, shift, 0, unroll=4)
        return carry

    lax.fori_loop(0, ROUNDS, one_round, 0)
    cells = (ROUNDS * ITERS, LANES)
    diagonal = lax.broadcasted_iota(jnp.int32, cells, 0) == lax.broadcasted_iota(jnp.int32, cells, 1)
    fin[...] = jnp.zeros_like(fin)
    for k in range(n):
        fin[k, :, 0:width] = (
            xs[ITERS, jnp.minimum(k + adv_ref[ROUNDS - 1], n - 1), 0:lat, :] if fused else xs[0, k, 0:lat, :])
        fin[k, 0:1, width:] = jnp.sum(jnp.where(diagonal, errs[k], 0.0), axis=0, keepdims=True)
    final_in[me] = fin[me]
    each_peer(lambda d: out_copy(d, me).start())
    each_peer(lambda d: out_copy(d, d).wait_recv(), near_first=True)
    sums = jnp.zeros((1, LANES), f32)
    for d in range(n):
        sums = sums + final_in[d, 0:1, width:]
        if direct:
            out_ref[0, :, d * pix:(d + 1) * pix] = final_in[d, :, 0:pix]
        else:
            out_ref[d] = final_in[d, :, 0:width]
    means = sums * (1.0 / (copies * lat * n * pix))
    for r in range(ROUNDS):
        err_ref[r] = means[:, r * ITERS:(r + 1) * ITERS]
    each_peer(lambda d: in_copy(d, me).wait_send())
    each_peer(lambda d: out_copy(d, me).wait_send())


def closing(final_ref, errors_ref, final_out, errors_out, sems):
    copies = [
        pltpu.make_async_copy(final_ref, final_out, sems.at[0]),
        pltpu.make_async_copy(errors_ref, errors_out, sems.at[1]),
    ]
    for copy in copies:
        copy.start()
    for copy in copies:
        copy.wait()


def shards(states, t_sched, advances, in_weight, time_weight, mid_weight, out_weight):
    n = lax.axis_size("steps")
    _, lat, rows = states.shape
    ch = mid_weight.shape[0]
    pix = rows // n
    direct = pix % LANES == 0
    width = round_up(pix, LANES)
    depth = round_up(XROWS + 3 * ROUNDS * n, LANES)
    fused = (
        n <= 16 and width == TILE and ch == TILE + LANES // 2 and depth == LANES
        and (n - ITERS + 1) // 2 > LAG_NOISE and 0 < VECTOR_ROWS < ch and 2 * lat == 8)
    vector_rows = VECTOR_ROWS if fused else 0
    if direct:
        sent = states
        out_shape = states.shape
    else:
        sent = jnp.pad(states.reshape(lat, n, pix).transpose(1, 0, 2), ((0, 0), (0, 0), (0, width - pix)))
        out_shape = sent.shape
    vmem = pl.BlockSpec(memory_space=pltpu.VMEM)
    hbm = pl.BlockSpec(memory_space=pltpu.HBM)
    f32, bf16 = jnp.float32, jnp.bfloat16
    final, errors = pl.pallas_call(
        functools.partial(kernel, n, pix, width, depth, direct, vector_rows, fused),
        out_shape=(pltpu.VMEM(out_shape, f32), pltpu.VMEM((ROUNDS, 1, ITERS), f32)),
        in_specs=[hbm] * 9,
        out_specs=(vmem, vmem),
        scratch_shapes=[
            pltpu.SMEM(t_sched.shape, jnp.int32),
            pltpu.SMEM(advances.shape, jnp.int32),
            pltpu.SMEM((TSTEPS,), f32),
            pltpu.VMEM(sent.shape, f32),
            pltpu.VMEM((lat, ch), bf16),
            pltpu.VMEM((lat, ch), bf16),
            pltpu.VMEM((ch, ch), f32),
            pltpu.VMEM((ch, ch), bf16),
            pltpu.VMEM((2 * ch, BASE), f32),
            pltpu.VMEM((n, lat, width), f32),
            pltpu.VMEM((ITERS + 1, n, 8, width), f32),
            pltpu.VMEM((n, lat, width + LANES), f32),
            pltpu.VMEM((n, lat, width + LANES), f32),
            pltpu.VMEM((n, ROUNDS * ITERS, LANES), f32),
            pltpu.VMEM((16 + ch - vector_rows, LANES + depth) if fused else (ch, depth), bf16),
            pltpu.VMEM((2, ch + 16, TILE) if fused else (ch, ch), bf16),
            pltpu.VMEM((16, ch), bf16),
            pltpu.VMEM((8, ch), f32),
            pltpu.VMEM((8, ch), f32),
            pltpu.VMEM((ROUNDS * n, 8, LANES), f32),
            pltpu.VMEM((ROUNDS * n, 8, LANES), f32),
            pltpu.VMEM((lat, max(vector_rows, 8), LANES), f32),
            pltpu.VMEM((ROUNDS * n, max(vector_rows, 8), LANES), f32),
            pltpu.VMEM((lat, 8, LANES), f32),
            pltpu.VMEM((ROUNDS * n, 8, LANES), f32),
            pltpu.VMEM((ROUNDS * n if fused else 1, depth - XROWS, LANES), bf16),
            pltpu.SemaphoreType.DMA((9,)),
        ] + [pltpu.SemaphoreType.DMA((n,))] * 4,
        compiler_params=pltpu.CompilerParams(
            collective_id=0, has_side_effects=True, vmem_limit_bytes=VMEM_BYTES),
        name="picard",
    )(*[pltpu.with_memory_space_constraint(held, pltpu.HBM) for held in (
        sent, t_sched, advances, jnp.asarray(alpha_table()), in_weight.T, out_weight, time_weight, mid_weight,
        jnp.asarray(trig_tables(time_weight.shape[1])))])
    final, errors = pl.pallas_call(
        closing,
        out_shape=(pltpu.HBM(out_shape, f32), pltpu.HBM((ROUNDS, 1, ITERS), f32)),
        in_specs=[vmem, vmem],
        out_specs=(hbm, hbm),
        scratch_shapes=[pltpu.SemaphoreType.DMA((2,))],
        compiler_params=pltpu.CompilerParams(vmem_limit_bytes=1 << 20),
        name="closing",
    )(pltpu.with_memory_space_constraint(final, pltpu.VMEM), pltpu.with_memory_space_constraint(errors, pltpu.VMEM))
    errors = errors.transpose(0, 2, 1)
    if not direct:
        final = final[:, :, :pix].transpose(1, 0, 2).reshape(states.shape)
    return final, errors


def solution(mesh):
    in_specs = (P(("groups", "steps"), None, None), P("groups"), P("groups"), P(), P(), P(), P())
    out_specs = (P(("groups", "steps"), None, None), P("groups", None, "steps"))
    return jax.shard_map(shards, mesh=mesh, in_specs=in_specs, out_specs=out_specs, check_vma=False)
```

```python
import functools
import math

import jax
import jax.numpy as jnp
import numpy as np
from jax import lax
from jax.experimental import pallas as pl
from jax.experimental.pallas import tpu as pltpu
from jax.sharding import PartitionSpec as P

TSTEPS = 1000
ITERS = 4
ROUNDS = 2
LANES = 128
BASE = 32
XROWS = 16
TILE = 256
LAG_MIXED = 1
LAG_NOISE = 3
VMEM_BYTES = 40 << 20
VECTOR_ROWS = 176


def alpha_table():
    levels = np.arange(TSTEPS, dtype=np.float64)
    low = math.sqrt(0.00085)
    high = math.sqrt(0.012)
    betas = (low + (high - low) * levels / (TSTEPS - 1)) ** 2
    return np.exp(np.cumsum(np.log1p(-betas))).astype(np.float32)


def trig_tables(width):
    half = width // 2
    freqs = np.exp(-math.log(10000.0) * np.arange(half, dtype=np.float64) / half)[:, None]
    digits = np.arange(BASE, dtype=np.float64)[None]
    high, low = freqs * digits * BASE, freqs * digits
    coarse = np.concatenate([np.cos(high), np.sin(high)]).astype(np.float32)
    fine = np.concatenate([np.cos(low), np.sin(low)]).astype(np.float32)
    return np.concatenate([coarse, fine])


def round_up(value, unit):
    return -(-value // unit) * unit


def kernel(
    n, pix, width, depth, direct, vector_rows, fused,
    states_hbm, sched_hbm, adv_hbm, alpha_hbm, inw_hbm, outw_hbm, timew_hbm, midw_hbm, trig_hbm,
    out_ref, err_ref,
    sched_ref, adv_ref, alpha_ref, states_ref, inw_ref, outw_ref, timew, midw, trig, xin, xs, fin, final_in, errs, lhs, mid, outs, outw, inw, coef_one, coef_two,
    in_table, time_table, linear_in, linear_time, hot_table,
    local, in_send, in_recv, out_send, out_recv,
):
    lat = outw_ref.shape[0]
    ch = midw.shape[0]
    me = lax.axis_index("steps")
    span = ROUNDS * n
    f32, bf16 = jnp.float32, jnp.bfloat16

    def peer(hop):
        if n > 16 or n & (n - 1):
            return lax.rem(me + hop, n)
        other = me
        for bit in range(n.bit_length() - 1):
            if hop >> bit & 1:
                digit = lax.rem(lax.div(me, 1 << bit), 2)
                other = other + (1 << bit) * (1 - 2 * digit)
        return other

    def source(d):
        if direct:
            return states_ref.at[0, :, pl.ds(pl.multiple_of(d * pix, LANES), pix)]
        return states_ref.at[d]

    def in_copy(d, slot):
        return pltpu.make_async_remote_copy(
            src_ref=source(d), dst_ref=xin.at[slot], send_sem=in_send.at[d], recv_sem=in_recv.at[slot],
            device_id={"steps": d}, device_id_type=pl.DeviceIdType.MESH)

    def out_copy(d, slot):
        return pltpu.make_async_remote_copy(
            src_ref=fin.at[d], dst_ref=final_in.at[slot], send_sem=out_send.at[d], recv_sem=out_recv.at[slot],
            device_id={"steps": d}, device_id_type=pl.DeviceIdType.MESH)

    def each_peer(act, near_first=False):
        if n <= 16:
            for hop in range(1, n) if near_first else reversed(range(1, n)):
                act(peer(hop))
        else:
            @pl.loop(1, n)
            def _(hop):
                act(peer(hop))

    loads = [
        pltpu.make_async_copy(source_ref, held, local.at[j])
        for j, (source_ref, held) in enumerate((
            (states_hbm, states_ref), (sched_hbm, sched_ref), (adv_hbm, adv_ref), (alpha_hbm, alpha_ref),
            (trig_hbm, trig), (timew_hbm, timew), (midw_hbm, midw), (inw_hbm, inw_ref), (outw_hbm, outw_ref)))
    ]
    loads[0].start()
    barrier = pltpu.get_barrier_semaphore()
    each_peer(lambda d: pl.semaphore_signal(
        barrier, inc=1, device_id={"steps": d}, device_id_type=pl.DeviceIdType.MESH))
    for load in loads[1:]:
        load.start()
    loads[0].wait()
    pl.semaphore_wait(barrier, n - 1)
    each_peer(lambda d: in_copy(d, me).start())

    for load in loads[1:4]:
        load.wait()
    lane = lax.broadcasted_iota(jnp.int32, (1, depth), 1) - XROWS
    member = jnp.where((lane >= 0) & (lane < 3 * span), lax.rem(jnp.maximum(lane, 0), span), -1)
    advance_one = adv_ref[0]

    def coefficients(m, stamps):
        place = jnp.where(m >= n, advance_one + m - n, m)
        now, after = sched_ref[place], sched_ref[place + 1]
        a_now = jnp.full((8, LANES), alpha_ref[now], f32)
        a_after = jnp.full((8, LANES), alpha_ref[after], f32)
        one = jnp.sqrt(a_after / a_now)
        two = jnp.sqrt(1.0 - a_after) - one * jnp.sqrt(1.0 - a_now)
        coef_one[m] = one - 1.0
        coef_two[m] = two
        return jnp.where(member == m, now, stamps)

    stamps = lax.fori_loop(0, span, coefficients, jnp.zeros((1, depth), jnp.int32), unroll=8)

    digit = lax.broadcasted_iota(jnp.int32, (BASE, depth), 0)
    hot_high = (digit == lax.shift_right_logical(stamps, 5)).astype(f32)
    hot_low = (digit == lax.bitwise_and(stamps, BASE - 1)).astype(f32)
    exact = lax.Precision.HIGHEST
    for load in loads[4:]:
        load.wait()
    high = jnp.dot(trig[0:ch], hot_high, precision=exact, preferred_element_type=f32)
    low = jnp.dot(trig[ch:], hot_low, precision=exact, preferred_element_type=f32)
    half = ch // 2
    cos_h, sin_h, cos_l, sin_l = high[:half], high[half:], low[:half], low[half:]
    feats = jnp.concatenate([cos_h * cos_l - sin_h * sin_l, sin_h * cos_l + cos_h * sin_l], axis=0)
    embed = jnp.dot(timew[...], feats, precision=exact, preferred_element_type=f32)
    inw[...] = jnp.zeros_like(inw)
    inw[0:lat, :] = inw_ref[...].astype(f32)
    unit = (lax.broadcasted_iota(jnp.int32, (8, depth), 0) == lane + XROWS).astype(f32)
    spread = lax.dot_general(
        inw[...], unit, (((0,), (0,)), ((), ())), precision=exact, preferred_element_type=f32)
    top = embed.astype(bf16).astype(f32)
    rest = embed - top
    middle = rest.astype(bf16).astype(f32)
    bottom = (rest - middle).astype(bf16).astype(f32)
    part = jnp.where(lane < span, top, jnp.where(lane < 2 * span, middle, bottom))
    part = jnp.where(member >= 0, part, 0.0)
    left = spread + part
    matrix_rows = ch - vector_rows
    outw[...] = jnp.zeros_like(outw)
    outw[0:lat, :] = outw_ref[...].astype(f32)
    half_mid = (midw[...].astype(f32) * 0.5).astype(bf16)
    whole = spread + jnp.where(member >= 0, embed, 0.0)
    linear = jnp.dot(outw[...], whole, precision=exact, preferred_element_type=f32)

    def folded(high, low):
        return jnp.concatenate([jnp.zeros_like(high), high + pltpu.roll(low, lat, axis=0)], axis=0).astype(bf16)

    padded_out = jnp.concatenate([outw[...], jnp.zeros_like(outw[...])], axis=0).astype(bf16)
    narrow = lambda rows, lanes: jnp.zeros((rows, lanes), bf16)
    cuts_one = (0, TILE - LANES // 2, ch)
    cuts_two = (0, LANES // 2, TILE - (ch - cuts_one[1]) + LANES // 2, ch)
    if fused:
        both_out = jnp.dot(padded_out, half_mid, preferred_element_type=f32)[0:8]
        both_top = both_out.astype(bf16).astype(f32)
        passed = folded(both_top, both_out - both_top)
        for part in range(2):
            one = half_mid[:, cuts_one[part]:cuts_one[part + 1]]
            two = padded_out[:, cuts_two[part]:cuts_two[part + 1]]
            mid[part, 0:ch, :] = jnp.concatenate([one, narrow(ch, two.shape[1])], axis=1)
            through = passed[:, cuts_one[part]:cuts_one[part + 1]]
            mid[part, ch:, :] = jnp.concatenate([through, two], axis=1)
        lhs[0:16, 0:LANES] = padded_out[:, cuts_two[2]:]
        line_top = linear.astype(bf16).astype(f32)
        line_rest = linear - line_top
        line_middle = line_rest.astype(bf16).astype(f32)
        line_bottom = line_rest - line_middle
        line = jnp.where(lane < span, line_top, jnp.where(lane < 2 * span, line_middle, line_bottom))
        lhs[0:16, LANES:] = folded(
            jnp.where((member >= 0) | (lane < 0), line, 0.0), jnp.where(lane < 0, line_middle, 0.0))
        lhs[16:, 0:LANES] = narrow(matrix_rows, LANES)
        lhs[16:, LANES:] = left[0:matrix_rows].astype(bf16)
    else:
        mid[...] = half_mid
        outs[...] = padded_out
        lhs[...] = left[0:matrix_rows].astype(bf16)
    for l in range(lat):
        if not fused:
            linear_in[l] = jnp.broadcast_to(linear[:, l:l + 1], (8, LANES))
        if vector_rows:
            in_table[l] = jnp.broadcast_to(whole[matrix_rows:, l:l + 1], (vector_rows, LANES))
    for m in range(span):
        at = XROWS + m
        if not fused:
            linear_time[m] = jnp.broadcast_to(linear[:, at:at + 1], (8, LANES))
        if vector_rows:
            time_table[m] = jnp.broadcast_to(whole[matrix_rows:, at:at + 1], (vector_rows, LANES))

    hot_row = lax.broadcasted_iota(jnp.int32, (depth - XROWS, LANES), 0)
    hot_member = jnp.where(hot_row < 3 * span, lax.rem(hot_row, span), -1)
    if fused:
        for m in range(span):
            hot_table[m] = (hot_member == m).astype(f32).astype(bf16)
    copies = 2 if fused else 1
    if not fused:
        xs[0] = jnp.zeros_like(xs[0])
    errs[...] = jnp.zeros_like(errs)

    def place(d, values):
        for copy in range(copies):
            xs[ITERS if fused else 0, d, copy * lat:(copy + 1) * lat, :] = values

    place(me, states_ref[0, :, pl.ds(pl.multiple_of(me * pix, LANES), pix)] if direct else states_ref[me])

    def arrived(d):
        in_copy(d, d).wait_recv()
        place(d, xin[d])

    each_peer(arrived, near_first=True)
    each_peer(lambda d: in_copy(d, me).wait_send())

    wide = lambda tile: jnp.concatenate([tile] * (width // LANES), axis=1) if width > LANES else tile

    def swish(full):
        return full * jax.nn.sigmoid(full)

    def bent(half):
        return half * jnp.tanh(half)

    join = lambda parts: parts[0] if len(parts) == 1 else jnp.concatenate(parts, axis=1)
    tiles = [slice(start, start + LANES) for start in range(0, width, LANES)]

    def affine(base, slopes, x, tile):
        total = base
        for l in range(lat):
            total = total + slopes[l] * x[l:l + 1, tile]
        return total

    def column(x, m):
        hot = wide(hot_table[m] if fused else (hot_member == m).astype(f32).astype(bf16))
        padded = jnp.concatenate([x, jnp.zeros((XROWS - 8, width), f32)], axis=0).astype(bf16)
        return jnp.concatenate([padded, hot], axis=0)

    def vector_part(x, m):
        rounded = x.astype(bf16).astype(f32)
        return join([swish(affine(time_table[m], in_table, rounded, tile).astype(bf16)) for tile in tiles])

    def linear_part(x, m):
        rounded = x.astype(bf16).astype(f32)
        return join([affine(linear_time[m], linear_in, rounded, tile) for tile in tiles])

    def product(weights, values):
        return jnp.dot(weights, values, preferred_element_type=f32)

    def note_error(row, k, change):
        square = change * change
        if pix < width:
            square = jnp.where(lax.broadcasted_iota(jnp.int32, square.shape, 1) < pix, square, 0.0)
        total = square[:, 0:LANES]
        for start in range(LANES, width, LANES):
            total = total + square[:, start:start + LANES]
        whole_sum = jnp.sum(jnp.sum(total, axis=0, keepdims=True), axis=1, keepdims=True)
        errs[k, pl.ds(row, 1), :] = jnp.broadcast_to(whole_sum, (1, LANES))

    def moved(r, m_at, old, noise):
        return wide(coef_one[m_at]) * old + wide(coef_two[m_at]) * noise

    def flat_round(r):
        todo = [(i, k) for i in range(ITERS) for k in range(i, n - 1)]
        groups = [todo[j:j + 2] for j in range(0, len(todo), 2)]
        count = len(groups)
        tails, hidden, late, running, straight = {}, {}, {}, {}, {}

        def finish(i, k, noise):
            row = r * ITERS + i
            old = xs[i, k]
            if k == i:
                running[i] = old
                xs[ITERS, k] = old
            running[i] = running[i] + moved(r, r * n + k, old, noise)
            note_error(row, k + 1, running[i] - xs[i, k + 1])
            xs[i + 1, k + 1] = running[i]

        def pad(values, lanes):
            return values if values.shape[1] == lanes else jnp.concatenate(
                [values, jnp.zeros((values.shape[0], lanes - values.shape[1]), bf16)], axis=1)

        for step in range(count + LAG_NOISE):
            new, second, third = step, step - LAG_MIXED, step - LAG_NOISE
            has_new, has_second, has_third = new < count, 0 <= second < count, 0 <= third < count
            sizes = [len(groups[g]) * width for g, there in ((new, has_new), (second, has_second), (third, has_third)) if there]
            lanes = max(sizes)
            noise = mixed = None
            if has_new:
                now, extras = [], []
                for i, k in groups[new]:
                    x = xs[i, k]
                    now.append(column(x, r * n + k))
                    extras.append(vector_part(x, r * n + k))
                new_rows = pad(join(now), lanes)
            else:
                new_rows = jnp.zeros((depth, lanes), bf16)
            old_rows = pad(late[third], lanes) if has_third else jnp.zeros((ch, lanes), bf16)
            mid_rows = pad(hidden[second], lanes) if has_second else jnp.zeros((ch, lanes), bf16)
            if has_new or has_third:
                end = lhs.shape[0] if has_new else 16
                both = product(lhs[0:end], jnp.concatenate([old_rows[cuts_two[2]:], new_rows], axis=0))
                if has_new:
                    tails[new] = both[8:16]
                    hid = swish(both[16:, 0:len(groups[new]) * width].astype(bf16))
                    hidden[new] = jnp.concatenate([hid, join(extras)], axis=0) if vector_rows else hid
                if has_third:
                    noise = both[0:8]
            if has_second or has_third:
                begin = 0 if has_second else ch
                for part in range(2):
                    values = jnp.concatenate([
                        mid_rows[cuts_one[part]:cuts_one[part + 1]], old_rows[cuts_two[part]:cuts_two[part + 1]]], axis=0)
                    both = product(mid[part, begin:], values)
                    if has_second:
                        mixed = both[0:ch] if mixed is None else mixed + both[0:ch]
                        line = both[ch + 8:ch + 16]
                        straight[second] = straight[second] + line if second in straight else line
                    if has_third:
                        noise = noise + both[ch - begin:ch - begin + 8]
            if has_second:
                late[second] = bent(mixed[:, 0:len(groups[second]) * width].astype(bf16))
                del hidden[second]
            if has_third:
                for j, (i, k) in enumerate(groups[third]):
                    at = slice(j * width, (j + 1) * width)
                    total = tails[third][:, at] + straight[third][:, at] + noise[:, at]
                    finish(i, k, total + pltpu.roll(total, lat, axis=0))
                del late[third]

    def rolled_round(r):
        for i in range(ITERS):
            row = r * ITERS + i

            def body(k, running):
                old = xs[0, k]
                tail = linear_part(old, r * n + k)
                hid = swish(product(lhs[...], column(old, r * n + k)).astype(bf16))
                half = product(mid[...], hid).astype(bf16)
                noise = tail + product(outs[...], half + bent(half))[0:8]
                note_error(row, k, running - old)
                xs[0, k] = running
                return running + moved(r, r * n + k, old, noise)

            running = lax.fori_loop(i, n - 1, body, xs[0, i])
            note_error(row, n - 1, running - xs[0, n - 1])
            xs[0, n - 1] = running

    def one_round(r, carry):
        advance = adv_ref[r]
        if fused:
            behind = jnp.where(r == 0, 0, adv_ref[jnp.maximum(r - 1, 0)])
            for k in range(n):
                xs[0, k] = xs[ITERS, jnp.minimum(k + behind, n - 1)]
            flat_round(r)
        else:
            rolled_round(r)

            def shift(k, carry):
                xs[0, k] = xs[0, jnp.minimum(k + advance, n - 1)]
                return carry

            lax.fori_loop(0, n, shift, 0, unroll=4)
        return carry

    lax.fori_loop(0, ROUNDS, one_round, 0)
    cells = (ROUNDS * ITERS, LANES)
    diagonal = lax.broadcasted_iota(jnp.int32, cells, 0) == lax.broadcasted_iota(jnp.int32, cells, 1)
    fin[...] = jnp.zeros_like(fin)
    for k in range(n):
        fin[k, :, 0:width] = (
            xs[ITERS, jnp.minimum(k + adv_ref[ROUNDS - 1], n - 1), 0:lat, :] if fused else xs[0, k, 0:lat, :])
        fin[k, 0:1, width:] = jnp.sum(jnp.where(diagonal, errs[k], 0.0), axis=0, keepdims=True)
    final_in[me] = fin[me]
    each_peer(lambda d: out_copy(d, me).start())
    each_peer(lambda d: out_copy(d, d).wait_recv(), near_first=True)
    sums = jnp.zeros((1, LANES), f32)
    for d in range(n):
        sums = sums + final_in[d, 0:1, width:]
        if direct:
            out_ref[0, :, d * pix:(d + 1) * pix] = final_in[d, :, 0:pix]
        else:
            out_ref[d] = final_in[d, :, 0:width]
    means = sums * (1.0 / (copies * lat * n * pix))
    for r in range(ROUNDS):
        err_ref[r] = means[:, r * ITERS:(r + 1) * ITERS]
    each_peer(lambda d: out_copy(d, me).wait_send())


def closing(final_ref, errors_ref, final_out, errors_out, sems):
    copies = [
        pltpu.make_async_copy(final_ref, final_out, sems.at[0]),
        pltpu.make_async_copy(errors_ref, errors_out, sems.at[1]),
    ]
    for copy in copies:
        copy.start()
    for copy in copies:
        copy.wait()


def shards(states, t_sched, advances, in_weight, time_weight, mid_weight, out_weight):
    n = lax.axis_size("steps")
    _, lat, rows = states.shape
    ch = mid_weight.shape[0]
    pix = rows // n
    direct = pix % LANES == 0
    width = round_up(pix, LANES)
    depth = round_up(XROWS + 3 * ROUNDS * n, LANES)
    fused = (
        n <= 16 and width == TILE and ch == TILE + LANES // 2 and depth == LANES
        and (n - ITERS + 1) // 2 > LAG_NOISE and 0 < VECTOR_ROWS < ch and 2 * lat == 8)
    vector_rows = VECTOR_ROWS if fused else 0
    if direct:
        sent = states
        out_shape = states.shape
    else:
        sent = jnp.pad(states.reshape(lat, n, pix).transpose(1, 0, 2), ((0, 0), (0, 0), (0, width - pix)))
        out_shape = sent.shape
    vmem = pl.BlockSpec(memory_space=pltpu.VMEM)
    hbm = pl.BlockSpec(memory_space=pltpu.HBM)
    f32, bf16 = jnp.float32, jnp.bfloat16
    final, errors = pl.pallas_call(
        functools.partial(kernel, n, pix, width, depth, direct, vector_rows, fused),
        out_shape=(pltpu.VMEM(out_shape, f32), pltpu.VMEM((ROUNDS, 1, ITERS), f32)),
        in_specs=[hbm] * 9,
        out_specs=(vmem, vmem),
        scratch_shapes=[
            pltpu.SMEM(t_sched.shape, jnp.int32),
            pltpu.SMEM(advances.shape, jnp.int32),
            pltpu.SMEM((TSTEPS,), f32),
            pltpu.VMEM(sent.shape, f32),
            pltpu.VMEM((lat, ch), bf16),
            pltpu.VMEM((lat, ch), bf16),
            pltpu.VMEM((ch, ch), f32),
            pltpu.VMEM((ch, ch), bf16),
            pltpu.VMEM((2 * ch, BASE), f32),
            pltpu.VMEM((n, lat, width), f32),
            pltpu.VMEM((ITERS + 1, n, 8, width), f32),
            pltpu.VMEM((n, lat, width + LANES), f32),
            pltpu.VMEM((n, lat, width + LANES), f32),
            pltpu.VMEM((n, ROUNDS * ITERS, LANES), f32),
            pltpu.VMEM((16 + ch - vector_rows, LANES + depth) if fused else (ch, depth), bf16),
            pltpu.VMEM((2, ch + 16, TILE) if fused else (ch, ch), bf16),
            pltpu.VMEM((16, ch), bf16),
            pltpu.VMEM((8, ch), f32),
            pltpu.VMEM((8, ch), f32),
            pltpu.VMEM((ROUNDS * n, 8, LANES), f32),
            pltpu.VMEM((ROUNDS * n, 8, LANES), f32),
            pltpu.VMEM((lat, max(vector_rows, 8), LANES), f32),
            pltpu.VMEM((ROUNDS * n, max(vector_rows, 8), LANES), f32),
            pltpu.VMEM((lat, 8, LANES), f32),
            pltpu.VMEM((ROUNDS * n, 8, LANES), f32),
            pltpu.VMEM((ROUNDS * n if fused else 1, depth - XROWS, LANES), bf16),
            pltpu.SemaphoreType.DMA((9,)),
        ] + [pltpu.SemaphoreType.DMA((n,))] * 4,
        compiler_params=pltpu.CompilerParams(
            collective_id=0, has_side_effects=True, vmem_limit_bytes=VMEM_BYTES),
        name="picard",
    )(*[pltpu.with_memory_space_constraint(held, pltpu.HBM) for held in (
        sent, t_sched, advances, jnp.asarray(alpha_table()), in_weight.T, out_weight, time_weight, mid_weight,
        jnp.asarray(trig_tables(time_weight.shape[1])))])
    final, errors = pl.pallas_call(
        closing,
        out_shape=(pltpu.HBM(out_shape, f32), pltpu.HBM((ROUNDS, 1, ITERS), f32)),
        in_specs=[vmem, vmem],
        out_specs=(hbm, hbm),
        scratch_shapes=[pltpu.SemaphoreType.DMA((2,))],
        compiler_params=pltpu.CompilerParams(vmem_limit_bytes=1 << 20),
        name="closing",
    )(pltpu.with_memory_space_constraint(final, pltpu.VMEM), pltpu.with_memory_space_constraint(errors, pltpu.VMEM))
    errors = errors.transpose(0, 2, 1)
    if not direct:
        final = final[:, :, :pix].transpose(1, 0, 2).reshape(states.shape)
    return final, errors


def solution(mesh):
    in_specs = (P(("groups", "steps"), None, None), P("groups"), P("groups"), P(), P(), P(), P())
    out_specs = (P(("groups", "steps"), None, None), P("groups", None, "steps"))
    return jax.shard_map(shards, mesh=mesh, in_specs=in_specs, out_specs=out_specs, check_vma=False)
```
